32 devices in a mesh: dp: 8 (over z, x), shard: 4 (over y, core).
Axes of the slice: x: 2, y: 2, z: 4, core: 2. Of those that a mesh axis runs over, the one named last changes fastest.
Arguments:
- hidden_in: bfloat16 [8192, 5120], P(('dp', 'shard')), may hold values from -6 to 6
- teacher: bfloat16 [8192, 768], P(('dp', 'shard')), may hold values from -6 to 6
- norm_gain: bfloat16 [5120], P('shard'), may hold values from 0.5 to 1.5
- w_key: bfloat16 [5120, 768], P('shard'), may hold values from -0.078125 to 0.078125
- group_rows: int32 [8], P('dp'), may hold values from 64 to 256
- member: int32 [8, 4], P('dp', 'shard'), may hold values from 0 to 1, as said below
Outputs:
- loss: float32 [], replicated
- grad_gain: float32 [5120], P('shard')
- grad_key: float32 [5120, 768], P('shard')
The draws below stay inside these ranges and needn't reach their ends.
Inputs may be any that keep to these rules, and one draw needn't show every extreme that they name: The first group_rows[p] token slots of each surviving device of group p hold valid tokens. `member`: 1 marks a surviving device; the first device of every group survives.
All inputs are finite; a program needn't handle non-finite values.
Results may differ from the reference program's by a relative error of at most 0.0023.
Values may be sent and summed in bfloat16 or wider, within the bound.
A program may use at most 128 MiB of HBM per device.

```python
import jax
import jax.numpy as jnp
from jax import lax

D = 5120
KV = 768
TOK_DEV = 256
GROUPS = 8
MEMBERS = 4
TOKENS = 8192


def draw_member(key, part):
    picks = jax.random.randint(key, (GROUPS, MEMBERS), 0, 4)
    first = jnp.arange(MEMBERS)[None, :] == 0
    return jnp.where((picks > 0) | first, 1, 0).astype(jnp.int32)


def touch_ends(values, key, low, top_value):
    longest = values.shape.index(max(values.shape))
    spots = []
    for shift in (0, 1):
        where = [jax.random.randint(jax.random.fold_in(key, axis), (), 0, length) for axis, length in enumerate(values.shape)]
        where[longest] = (where[longest] + shift) % values.shape[longest]
        spots.append(tuple(where))
    return values.at[spots[0]].set(low).at[spots[1]].set(top_value)


def strengthened(drawn, key, source, target, blocks, factor):
    owner, partner = [(jnp.arange(drawn.shape[dim]) // (drawn.shape[dim] // blocks)).reshape([-1 if axis == dim else 1 for axis in range(drawn.ndim)]) for dim in (source, target)]
    chosen = jax.random.permutation(key, blocks)[partner]
    strong = (owner == chosen) | (owner == (partner + blocks // 2) % blocks)
    return jnp.where(strong, factor * drawn, drawn)


def block_scale(rng, dims, cuts, smallest, high):
    gain, own = 1.0, jax.random.fold_in(rng, 6)
    for dim, shards_of in cuts:
        draws = jnp.exp(jax.random.uniform(jax.random.fold_in(own, dim), (shards_of,), jnp.float32, smallest / len(cuts), high / len(cuts)))
        gain = gain * jnp.repeat(draws, dims[dim] // shards_of).reshape([-1 if axis == dim else 1 for axis in range(len(dims))])
    return gain


def noise(rng, shape, deviation, limit, cuts=(), dtype=jnp.bfloat16):
    result = deviation * jax.random.normal(rng, shape, jnp.float32)
    if cuts:
        result = result * block_scale(rng, shape, cuts, -0.22, 0.18)
    return jnp.clip(result, -limit, limit).astype(dtype)


def noise_with(rng, extent, deviation, limit, pieces, heavy, held_as=jnp.bfloat16):
    values = deviation * jax.random.normal(rng, extent, jnp.float32)
    if pieces:
        values = values * block_scale(rng, extent, pieces, -0.22, 0.18)
    return jnp.clip(strengthened(values, jax.random.fold_in(rng, 3), *heavy), -limit, limit).astype(held_as)


def setup_inputs(seed: int = 0) -> dict:
    seeds = jax.random.split(jax.random.key(seed), 7)
    return {
        "hidden_in": noise_with(seeds[0], (TOKENS, D), 1.0, 6.0, ((0, 32),), (0, 1, 32, 2.75)),
        "teacher": noise(seeds[1], (TOKENS, KV), 1.0, 6.0, ((0, 32),)),
        "norm_gain": jnp.clip(1.0 + 0.1 * jax.random.normal(seeds[2], (D,), jnp.float32), 0.5, 1.5).astype(jnp.bfloat16),
        "w_key": noise(seeds[3], (D, KV), D ** -0.5, 0.078125, ((0, 4),)),
        "group_rows": touch_ends(jax.random.randint(seeds[4], (GROUPS,), TOK_DEV // 4, TOK_DEV + 1), jax.random.fold_in(seeds[4], 1), TOK_DEV // 4, TOK_DEV).astype(jnp.int32),
        "member": draw_member(jax.random.fold_in(seeds[6], 71), 0),
    }


EPSILON = 1e-06
SCALE = 1024.0

def reference(hidden_in, teacher, norm_gain, w_key, group_rows, member):
    blocks = GROUPS * MEMBERS
    live_rows = jnp.repeat(group_rows, MEMBERS).astype(jnp.int32)
    alive = member.reshape(blocks).astype(jnp.int32)
    total_count = jnp.sum(member.astype(jnp.float32) * group_rows.astype(jnp.float32)[:, None])
    gains = norm_gain.astype(jnp.float32)

    def one_block(carry, inputs):
        loss_sum, gain_acc, key_acc = carry
        block_in, block_teacher, block_rows, block_alive = inputs
        position = lax.broadcasted_iota(jnp.int32, (TOK_DEV, 1), 0)
        valid = jnp.where((position < block_rows) & (block_alive == 1), 1.0, 0.0).astype(jnp.float32)
        values = block_in.astype(jnp.float32)
        inverse_rms = lax.rsqrt(lax.optimization_barrier(jnp.mean(values * values, axis=1, keepdims=True)) + EPSILON)
        scaled = values * inverse_rms
        normed = (scaled * gains).astype(jnp.bfloat16)
        keys = jnp.dot(normed, w_key, preferred_element_type=jnp.float32)
        diff = keys - block_teacher.astype(jnp.float32)
        loss_sum = loss_sum + jnp.sum(valid * diff * diff)
        upstream = (SCALE / total_count * valid * diff).astype(jnp.bfloat16)
        term_key = jnp.dot(normed.T, upstream, preferred_element_type=jnp.float32)
        dnormed = jnp.dot(upstream, w_key.T, preferred_element_type=jnp.float32)
        term_gain = lax.optimization_barrier(jnp.sum(dnormed * scaled, axis=0))
        return ((loss_sum, gain_acc + term_gain, key_acc + term_key), None)
    start = (jnp.zeros((), jnp.float32), jnp.zeros((D,), jnp.float32), jnp.zeros((D, KV), jnp.float32))
    inputs = (hidden_in.reshape(blocks, TOK_DEV, D), teacher.reshape(blocks, TOK_DEV, KV), live_rows, alive)
    final, unused = lax.scan(one_block, start, inputs)
    loss_sum, gain_acc, key_acc = final
    loss = loss_sum / (2.0 * KV * total_count)
    return (loss, gain_acc, key_acc)
```

```python
import functools
import math

import jax
import jax.numpy as jnp
from jax import lax
from jax.experimental import pallas as pl
from jax.experimental.pallas import tpu as pltpu
from jax.sharding import PartitionSpec as P

EPSILON = 1e-06
SCALE = 1024.0
MESH = pl.DeviceIdType.MESH
F32 = jnp.float32
BF16 = jnp.bfloat16


def inner_of(groups):
    return max(d for d in range(1, groups + 1) if groups % d == 0 and d * d <= groups)


def paired(index, k, size):
    if size & (size - 1):
        return None
    out, bit = 0, 1
    while bit < size:
        out = out + lax.rem(lax.rem(index // bit, 2) + (k // bit) % 2, 2) * bit
        bit *= 2
    return out


def kernel(
    members, groups, width, chunks,
    live_rows, alive, hidden_in, teacher, gains, w_in,
    out, loss_out,
    hidden, w_full, gains_all, cnt_m, cnt_g, loss_m, loss_g,
    n_own, n_recv, n_t, dk_all, grads,
    x_send, x_recv, z_near, z_near_recv, z_far, z_far_recv,
    load_s, gain_s, gain_r, cnt_s, cnt_r, cntg_s, cntg_r,
    loss_s, loss_r, lossg_s, lossg_r, wy_s, wy_r, wz_s, wz_r, wx_s, wx_r, wt_s, wt_r,
    n_s, n_r, dk_s, dk_r, dks_s, dks_r, dkf_s, dkf_r,
    x_s, x_r, z_s, z_r, az_s, az_r, ax_s, ax_r,
):
    tokens, kv = teacher.shape
    feats = w_in.shape[0]
    kc = kv // chunks
    inner = inner_of(groups)
    outer = groups // inner
    hrows = feats // inner
    qrows = hrows // outer
    pairs = members // 2
    p, s = lax.axis_index("dp"), lax.axis_index("shard")
    px, pz = lax.rem(p, inner), p // inner
    chip, par = s // 2, lax.rem(s, 2)
    twin = chip * 2 + 1 - par
    pending = []

    def member_at(d):
        return lax.rem(s + d, members)

    def group_at(d):
        return lax.rem(p + d, groups)

    def chip_at(d):
        return lax.rem(chip + d + pairs, pairs)

    def x_at(d):
        return lax.rem(px + d + inner, inner)

    def z_to(k):
        q = paired(pz, k, outer)
        return lax.rem(pz + k, outer) if q is None else q

    def z_from(k):
        q = paired(pz, k, outer)
        return lax.rem(pz + outer - k, outer) if q is None else q

    def send(src, dst, ssem, rsem, group, member):
        copy = pltpu.make_async_remote_copy(
            src_ref=src, dst_ref=dst, send_sem=ssem, recv_sem=rsem,
            device_id=(group, member), device_id_type=MESH,
        )
        copy.start()
        pending.append(copy)

    def arrived(dst, ssem, rsem):
        pltpu.make_async_remote_copy(
            src_ref=dst, dst_ref=dst, send_sem=ssem, recv_sem=rsem,
            device_id=(p, twin), device_id_type=MESH,
        ).wait_recv()

    def lanes_of(c):
        return pl.ds(c * kc, kc)

    def rows_at(x, z):
        return pl.ds(pl.multiple_of(x * hrows + z * qrows, 16), qrows)

    loads = [
        pltpu.make_async_copy(w_in.at[:, lanes_of(c)], w_full.at[c, s], load_s.at[c])
        for c in range(chunks)
    ]
    loads.append(pltpu.make_async_copy(hidden_in, hidden, load_s.at[chunks]))
    for copy in loads:
        copy.start()

    rows_count, is_alive = live_rows[0], alive[0, 0]
    gains_all[s] = gains[...]
    cnt_m[s] = jnp.broadcast_to((is_alive * rows_count).astype(F32), (8, 128))

    barrier = pltpu.get_barrier_semaphore()
    for d in range(1, members):
        pl.semaphore_signal(barrier, inc=1, device_id=(p, member_at(d)), device_id_type=MESH)
    for d in range(1, groups):
        pl.semaphore_signal(barrier, inc=1, device_id=(group_at(d), s), device_id_type=MESH)
    pl.semaphore_wait(barrier, members + groups - 2)

    def to_members(buf, ssem, rsem):
        for d in range(1, members):
            send(buf.at[s], buf.at[s], ssem.at[d - 1], rsem.at[d - 1], p, member_at(d))

    def from_members(buf, ssem, rsem):
        for d in range(1, members):
            j = lax.rem(s + members - d, members)
            arrived(buf.at[j], ssem.at[d - 1], rsem.at[d - 1])

    def to_groups(buf, ssem, rsem):
        for d in range(1, groups):
            send(buf.at[p], buf.at[p], ssem.at[d - 1], rsem.at[d - 1], group_at(d), s)

    def from_groups(buf, ssem, rsem):
        for d in range(1, groups):
            j = lax.rem(p + groups - d, groups)
            arrived(buf.at[j], ssem.at[d - 1], rsem.at[d - 1])

    def total_of(buf, n):
        value = buf[0]
        for i in range(1, n):
            value = value + buf[i]
        return value

    def spread(spot_of, c, zs, zr, xs, xr):
        spot = spot_of(px, pz)
        for k in range(1, outer):
            send(spot, spot, zs.at[c, k - 1], zr.at[c, k - 1], z_to(k) * inner + px, s)
        for e in range(1, inner):
            send(spot, spot, xs.at[c, e - 1, 0], xr.at[c, e - 1, 0], pz * inner + x_at(e), s)

    def relay(spot_of, c, zs, zr, xs, xr):
        for k in range(1, outer):
            spot = spot_of(px, z_from(k))
            arrived(spot, zs.at[c, k - 1], zr.at[c, k - 1])
            for e in range(1, inner):
                send(spot, spot, xs.at[c, e - 1, k], xr.at[c, e - 1, k], pz * inner + x_at(e), s)

    def settle(spot_of, c, xs, xr):
        for k in range(outer):
            for e in range(1, inner):
                q = z_from(k) if k else pz
                arrived(spot_of(x_at(-e), q), xs.at[c, e - 1, k], xr.at[c, e - 1, k])

    to_members(gains_all, gain_s, gain_r)
    to_members(cnt_m, cnt_s, cnt_r)

    def w_spot(c, j):
        return lambda x, z: w_full.at[c, j, rows_at(x, z), :]

    def w_own(c):
        loads[c].wait()
        spot = w_spot(c, s)(px, pz)
        for d in range(1, pairs):
            send(spot, spot, wy_s.at[c, d - 1], wy_r.at[c, d - 1], p, chip_at(d) * 2 + par)
        send(w_full.at[c, s], w_full.at[c, s], wt_s.at[c, 0], wt_r.at[c, 0], p, twin)

    def w_index(c, d):
        return c * (pairs - 1) + d - 1

    def w_spread(c):
        for d in range(1, pairs):
            spot = w_spot(c, chip_at(-d) * 2 + par)
            arrived(spot(px, pz), wy_s.at[c, d - 1], wy_r.at[c, d - 1])
            spread(spot, w_index(c, d), wz_s, wz_r, wx_s, wx_r)

    def w_relay(c):
        for d in range(1, pairs):
            relay(w_spot(c, chip_at(-d) * 2 + par), w_index(c, d), wz_s, wz_r, wx_s, wx_r)

    def w_settle(c):
        for d in range(1, pairs):
            j = chip_at(-d) * 2 + par
            settle(w_spot(c, j), w_index(c, d), wx_s, wx_r)
            send(w_full.at[c, j], w_full.at[c, j], wt_s.at[c, d], wt_r.at[c, d], p, twin)

    def w_ready(c):
        for d in range(pairs):
            j = chip_at(-d) * 2 + 1 - par
            arrived(w_full.at[c, j], wt_s.at[c, d], wt_r.at[c, d])

    for c in range(chunks):
        w_own(c)

    def half_of(e):
        return pl.ds(pl.multiple_of(x_at(e) * hrows, 128), hrows)

    def n_index(d, h):
        return ((d - 1) * 2 + h) * inner

    loads[chunks].wait()
    step_rows = 32
    from_members(gains_all, gain_s, gain_r)

    def normalise(r, carry):
        rows = pl.ds(pl.multiple_of(r * step_rows, step_rows), step_rows)
        square = jnp.zeros((step_rows, 1), F32)
        for j in range(members):
            x = hidden[rows, pl.ds(j * feats, feats)].astype(F32)
            square = square + jnp.sum(x * x, axis=1, keepdims=True)
        inv = lax.rsqrt(square / width + EPSILON)
        for j in range(members):
            x = hidden[rows, pl.ds(j * feats, feats)].astype(F32)
            n_own[j, rows, :] = (x * inv * gains_all[j]).astype(BF16)
        return carry
    lax.fori_loop(0, tokens // step_rows, normalise, 0)

    def n_send(e):
        for d in range(1, pairs):
            for h in range(2):
                j = chip_at(d) * 2 + lax.rem(par + h, 2)
                i = n_index(d, h) + e
                send(n_own.at[j, :, half_of(e)], n_recv.at[s, :, half_of(e)], n_s.at[i], n_r.at[i], p, j)

    for e in range(1, inner):
        n_send(e)
    t_slot = (pairs - 1) * 2 * inner
    send(n_own.at[twin], n_recv.at[s], n_s.at[t_slot], n_r.at[t_slot], p, twin)

    def turn(source, m, first, count):
        def step(b, carry):
            lanes = pl.ds(pl.multiple_of(first + b * 128, 128), 128)
            n_t[lanes, pl.ds(pl.multiple_of(m * tokens, 128), tokens)] = source[:, lanes].T
            return carry
        lax.fori_loop(0, count // 128, step, 0)

    def n_land(e):
        for d in range(1, pairs):
            for h in range(2):
                m = chip_at(-d) * 2 + lax.rem(par + h, 2)
                i = n_index(d, h) + e
                arrived(n_recv.at[m, :, half_of(e)], n_s.at[i], n_r.at[i])
                turn(n_recv.at[m], m, x_at(e) * hrows, hrows)

    w_spread(0)
    turn(n_own.at[s], s, 0, feats)
    from_members(cnt_m, cnt_s, cnt_r)
    cnt_g[p] = total_of(cnt_m, members)
    to_groups(cnt_g, cntg_s, cntg_r)
    w_spread(1 % chunks) if chunks > 1 else None
    w_relay(0)
    arrived(n_recv.at[twin], n_s.at[t_slot], n_r.at[t_slot])
    turn(n_recv.at[twin], twin, 0, feats)
    for c in range(2, chunks):
        w_spread(c)
        w_relay(c - 1)
        w_settle(c - 2)
    if chunks > 1:
        w_relay(chunks - 1)

    from_groups(cnt_g, cntg_s, cntg_r)
    total = total_of(cnt_g, groups)
    position = lax.broadcasted_iota(jnp.int32, (tokens, 1), 0)
    valid = jnp.where(position < rows_count * is_alive, 1.0, 0.0).astype(F32)
    scale = valid * (SCALE / total[:1, :1])

    def stage_keys(c, loss):
        w_ready(c)
        keys = jnp.dot(n_own[0], w_full[c, 0], preferred_element_type=F32)
        for j in range(1, members):
            keys = keys + jnp.dot(n_own[j], w_full[c, j], preferred_element_type=F32)
        diff = keys - teacher[:, lanes_of(c)].astype(F32)
        dk_all[c, s] = (scale * diff).astype(BF16)
        for d in range(1, pairs):
            send(
                dk_all.at[c, s], dk_all.at[c, s], dk_s.at[c, d - 1], dk_r.at[c, d - 1],
                p, chip_at(d) * 2 + par,
            )
        send(dk_all.at[c, s], dk_all.at[c, s], dks_s.at[c], dks_r.at[c], p, twin)
        return loss + jnp.sum(valid * diff * diff, axis=0, keepdims=True)

    def dk_pass(c):
        for d in range(1, pairs):
            q = chip_at(-d) * 2 + par
            arrived(dk_all.at[c, q], dk_s.at[c, d - 1], dk_r.at[c, d - 1])
            send(dk_all.at[c, q], dk_all.at[c, q], dkf_s.at[c, d - 1], dkf_r.at[c, d - 1], p, twin)

    def dk_ready(c):
        arrived(dk_all.at[c, twin], dks_s.at[c], dks_r.at[c])
        for d in range(1, pairs):
            q = chip_at(-d) * 2 + 1 - par
            arrived(dk_all.at[c, q], dkf_s.at[c, d - 1], dkf_r.at[c, d - 1])

    def product(c, e):
        dk = dk_all[c].reshape(members * tokens, kc)
        return jnp.dot(n_t[half_of(e), :], dk, preferred_element_type=F32)

    def stage_x(c):
        dk_ready(c)
        for e in range(1, inner):
            x_send[c, e - 1] = product(c, e).astype(BF16)
            send(
                x_send.at[c, e - 1], x_recv.at[c, e - 1], x_s.at[c, e - 1], x_r.at[c, e - 1],
                pz * inner + x_at(e), s,
            )

    def quarter(z):
        return pl.ds(pl.multiple_of(z * qrows, 16), qrows)

    def stage_z(c):
        grads[c] = product(c, 0)
        for e in range(1, inner):
            arrived(x_recv.at[c, e - 1], x_s.at[c, e - 1], x_r.at[c, e - 1])
        def sum_of(rows):
            value = grads[c, rows, :]
            for e in range(1, inner):
                value = value + x_recv[c, e - 1, rows, :].astype(F32)
            return value
        for k in range(1, outer):
            to = z_to(k)
            value = sum_of(quarter(to))
            if k == 1:
                z_near[c] = value
                src, dst = z_near.at[c], z_near_recv.at[c]
            else:
                z_far[c, k - 2] = value.astype(BF16)
                src, dst = z_far.at[c, k - 2], z_far_recv.at[c, k - 2]
            send(src, dst, z_s.at[c, k - 1], z_r.at[c, k - 1], to * inner + px, s)
        grads[c, quarter(pz), :] = sum_of(quarter(pz))

    def out_spot(c):
        return lambda x, z: out.at[rows_at(x, z), lanes_of(c)]

    def stage_sum(c):
        value = grads[c, quarter(pz), :]
        for k in range(1, outer):
            dst = z_near_recv.at[c] if k == 1 else z_far_recv.at[c, k - 2]
            arrived(dst, z_s.at[c, k - 1], z_r.at[c, k - 1])
            value = value + dst[...].astype(F32)
        out[rows_at(px, pz), lanes_of(c)] = value.astype(BF16)
        spread(out_spot(c), c, az_s, az_r, ax_s, ax_r)

    def stage_relay(c):
        relay(out_spot(c), c, az_s, az_r, ax_s, ax_r)

    loss = jnp.zeros((1, kc), F32)
    for c in range(max(chunks - 2, 0), chunks):
        if c == max(chunks - 2, 0):
            w_settle(c) if chunks > 1 else w_settle(0)
            for b in range(c):
                loss = stage_keys(b, loss)
        else:
            w_settle(c)
    for c in range(max(chunks - 2, 0), chunks):
        loss = stage_keys(c, loss)
    loss_m[s] = jnp.broadcast_to(jnp.sum(loss, axis=1, keepdims=True), (8, 128))
    to_members(loss_m, loss_s, loss_r)
    n_send(0)

    for e in range(1, inner):
        n_land(e)
    for c in range(chunks):
        dk_pass(c)
        stage_x(c)
    n_land(0)
    from_members(loss_m, loss_s, loss_r)
    loss_g[p] = total_of(loss_m, members)
    to_groups(loss_g, lossg_s, lossg_r)
    for step in range(chunks + 2):
        for lag, stage in enumerate((stage_z, stage_sum, stage_relay)):
            c = step - lag
            if 0 <= c < chunks:
                stage(c)
    from_groups(loss_g, lossg_s, lossg_r)
    loss_out[...] = total_of(loss_g, groups) / (2.0 * kv * total)
    for c in range(chunks):
        settle(out_spot(c), c, ax_s, ax_r)
    for copy in pending:
        copy.wait_send()


def body(members, groups, hidden_in, teacher, norm_gain, w_key, group_rows, member):
    tokens, width = hidden_in.shape
    owned, kv = w_key.shape
    inner = inner_of(groups)
    outer = groups // inner
    unit = math.lcm(128 * inner, 16 * groups)
    feats = -(-owned // unit) * unit
    chunks = kv // 256 if kv % 256 == 0 else 1
    kc = kv // chunks
    gains = norm_gain.astype(F32)
    hidden, weights, wide_gains = hidden_in, w_key, gains
    if feats != owned:
        extra = feats - owned
        hidden = jnp.pad(hidden_in.reshape(tokens, members, owned), ((0, 0), (0, 0), (0, extra)))
        hidden = hidden.reshape(tokens, members * feats)
        weights = jnp.pad(w_key, ((0, extra), (0, 0)))
        wide_gains = jnp.pad(gains, (0, extra))
    hrows, pairs = feats // inner, members // 2
    qrows = hrows // outer
    vm = pltpu.VMEM

    def some(n):
        return max(n, 1)

    def sems(*shape):
        kind = pltpu.SemaphoreType.DMA(tuple(some(n) for n in shape))
        return [kind, kind]

    small = lambda n: vm((n, 8, 128), F32)
    space = pltpu.MemorySpace
    grad, loss = pl.pallas_call(
        functools.partial(kernel, members, groups, width, chunks),
        out_shape=(
            jax.ShapeDtypeStruct((feats, kv), BF16),
            jax.ShapeDtypeStruct((8, 128), F32),
        ),
        in_specs=[
            pl.BlockSpec(memory_space=pltpu.SMEM),
            pl.BlockSpec(memory_space=pltpu.SMEM),
            pl.BlockSpec(memory_space=pl.ANY),
            pl.BlockSpec(memory_space=pltpu.VMEM),
            pl.BlockSpec(memory_space=pltpu.VMEM),
            pl.BlockSpec(memory_space=pl.ANY),
        ],
        out_specs=(pl.BlockSpec(memory_space=pltpu.VMEM),) * 2,
        scratch_shapes=[
            vm((tokens, members * feats), BF16),
            vm((chunks, members, feats, kc), BF16),
            vm((members, 1, feats), F32),
            small(members), small(groups), small(members), small(groups),
            vm((members, tokens, feats), BF16), vm((members, tokens, feats), BF16),
            vm((feats, members * tokens), BF16),
            vm((chunks, members, tokens, kc), BF16),
            vm((chunks, hrows, kc), F32),
            vm((chunks, some(inner - 1), hrows, kc), BF16), vm((chunks, some(inner - 1), hrows, kc), BF16),
            vm((chunks, qrows, kc), F32), vm((chunks, qrows, kc), F32),
            vm((chunks, some(outer - 2), qrows, kc), BF16), vm((chunks, some(outer - 2), qrows, kc), BF16),
            sems(chunks + 1)[0],
            *sems(members - 1), *sems(members - 1), *sems(groups - 1),
            *sems(members - 1), *sems(groups - 1),
            *sems(chunks, pairs - 1),
            *sems(chunks * (pairs - 1), outer - 1), *sems(chunks * (pairs - 1), inner - 1, outer),
            *sems(chunks, pairs),
            *sems((pairs - 1) * 2 * inner + 1),
            *sems(chunks, pairs - 1), *sems(chunks), *sems(chunks, pairs - 1),
            *sems(chunks, inner - 1), *sems(chunks, outer - 1),
            *sems(chunks, outer - 1), *sems(chunks, inner - 1, outer),
        ],
        compiler_params=pltpu.CompilerParams(
            collective_id=0, has_side_effects=True, vmem_limit_bytes=60 * 1024 * 1024
        ),
    )(group_rows, member, hidden, teacher, wide_gains.reshape(1, feats), weights)
    grad_key = grad[:owned].astype(F32)
    grad_gain = jnp.sum(grad_key * w_key.astype(F32), axis=1) / gains
    return (loss[0, 0], grad_gain, grad_key)


def solution(mesh):
    in_specs = (
        P(("dp", "shard"), None),
        P(("dp", "shard"), None),
        P("shard"),
        P("shard", None),
        P("dp"),
        P("dp", "shard"),
    )
    out_specs = (P(), P("shard"), P("shard", None))
    step = functools.partial(body, mesh.shape["shard"], mesh.shape["dp"])
    return jax.shard_map(step, mesh=mesh, in_specs=in_specs, out_specs=out_specs, check_vma=False)
```

```python
import functools
import math

import jax
import jax.numpy as jnp
from jax import lax
from jax.experimental import pallas as pl
from jax.experimental.pallas import tpu as pltpu
from jax.sharding import PartitionSpec as P

EPSILON = 1e-06
SCALE = 1024.0
MESH = pl.DeviceIdType.MESH
F32 = jnp.float32
BF16 = jnp.bfloat16


def inner_of(groups):
    return max(d for d in range(1, groups + 1) if groups % d == 0 and d * d <= groups)


def blocks_of(rows):
    unit = 128
    count = rows // unit
    sizes = []
    while count > 0:
        size = 2 if count > 2 else count if count < 2 or not sizes else 1
        sizes.append(size * unit)
        count -= size
    return sizes


AFTER_KEYS, KEYS_AHEAD, KEYS_STEP = 2, 2, 1
LAGS, X_FIRST = (0, 2, 4, 6, 8), False
TUNED = ((0, 0), (0, 1), None, (1, 0), (1, 1), (0, 2), (1, 2), (2, 0), (2, 1), (2, 2))


def plan_of(blocks, chunks):
    if (blocks, chunks) == (3, 3):
        return TUNED
    return [(b, c) for c in range(chunks) for b in range(blocks)]


def paired(index, k, size):
    if size & (size - 1):
        return None
    out, bit = 0, 1
    while bit < size:
        out = out + lax.rem(lax.rem(index // bit, 2) + (k // bit) % 2, 2) * bit
        bit *= 2
    return out


def kernel(
    members, groups, width, chunks, blocks,
    live_rows, alive, hidden_in, teacher, gains, w_in,
    out, loss_out,
    hidden, w_full, gains_all, cnt_m, cnt_g, loss_m, loss_g,
    n_own, n_recv, n_t, dk_all, grads,
    x_send, x_recv, z_near, z_near_recv, z_far, z_far_recv, z_own,
    load_s, gain_s, gain_r, cnt_s, cnt_r, cntg_s, cntg_r,
    loss_s, loss_r, lossg_s, lossg_r, wy_s, wy_r, wz_s, wz_r, wx_s, wx_r, wt_s, wt_r,
    n_s, n_r, dk_s, dk_r, dks_s, dks_r, dkf_s, dkf_r,
    x_s, x_r, z_s, z_r, az_s, az_r, af_s, af_r, ax_s, ax_r,
):
    tokens, kv = teacher.shape
    feats = w_in.shape[0]
    kc = kv // chunks
    inner = inner_of(groups)
    outer = groups // inner
    hrows = feats // inner
    qrows = hrows // outer
    pairs = members // 2
    starts = [sum(blocks[:b]) for b in range(len(blocks))]
    p, s = lax.axis_index("dp"), lax.axis_index("shard")
    px, pz = lax.rem(p, inner), p // inner
    chip, par = s // 2, lax.rem(s, 2)
    twin = chip * 2 + 1 - par
    pending = []

    def scoped(stage):
        def run(c, *rest):
            with jax.named_scope("_".join([stage.__name__, str(c), *[str(r) for r in rest if isinstance(r, int)]])):
                return stage(c, *rest)
        return run

    def member_at(d):
        return lax.rem(s + d, members)

    def group_at(d):
        return lax.rem(p + d, groups)

    def chip_at(d):
        return lax.rem(chip + d + pairs, pairs)

    def x_at(d):
        return lax.rem(px + d + inner, inner)

    def z_to(k):
        q = paired(pz, k, outer)
        return lax.rem(pz + k, outer) if q is None else q

    def z_from(k):
        q = paired(pz, k, outer)
        return lax.rem(pz + outer - k, outer) if q is None else q

    def send(src, dst, ssem, rsem, group, member):
        copy = pltpu.make_async_remote_copy(
            src_ref=src, dst_ref=dst, send_sem=ssem, recv_sem=rsem,
            device_id=(group, member), device_id_type=MESH,
        )
        copy.start()
        pending.append(copy)

    def arrived(dst, ssem, rsem):
        pltpu.make_async_remote_copy(
            src_ref=dst, dst_ref=dst, send_sem=ssem, recv_sem=rsem,
            device_id=(p, twin), device_id_type=MESH,
        ).wait_recv()

    def lanes_of(c):
        return pl.ds(c * kc, kc)

    def rows_at(x, z):
        return pl.ds(pl.multiple_of(x * hrows + z * qrows, 16), qrows)

    loads = [
        pltpu.make_async_copy(w_in.at[:, lanes_of(c)], w_full.at[c, s], load_s.at[c])
        for c in range(chunks)
    ]
    loads.append(pltpu.make_async_copy(hidden_in, hidden, load_s.at[chunks]))
    for copy in loads:
        copy.start()

    rows_count, is_alive = live_rows[0], alive[0, 0]
    gains_all[s] = gains[...].astype(F32).reshape(1, feats)
    cnt_m[s] = jnp.broadcast_to((is_alive * rows_count).astype(F32), (8, 128))

    barrier = pltpu.get_barrier_semaphore()
    for d in range(1, members):
        pl.semaphore_signal(barrier, inc=1, device_id=(p, member_at(d)), device_id_type=MESH)
    for d in range(1, groups):
        pl.semaphore_signal(barrier, inc=1, device_id=(group_at(d), s), device_id_type=MESH)
    pl.semaphore_wait(barrier, members + groups - 2)

    def to_members(buf, ssem, rsem):
        for d in range(1, members):
            send(buf.at[s], buf.at[s], ssem.at[d - 1], rsem.at[d - 1], p, member_at(d))

    def from_members(buf, ssem, rsem):
        for d in range(1, members):
            j = lax.rem(s + members - d, members)
            arrived(buf.at[j], ssem.at[d - 1], rsem.at[d - 1])

    def to_groups(buf, ssem, rsem):
        for d in range(1, groups):
            send(buf.at[p], buf.at[p], ssem.at[d - 1], rsem.at[d - 1], group_at(d), s)

    def from_groups(buf, ssem, rsem):
        for d in range(1, groups):
            j = lax.rem(p + groups - d, groups)
            arrived(buf.at[j], ssem.at[d - 1], rsem.at[d - 1])

    def total_of(buf, n):
        value = buf[0]
        for i in range(1, n):
            value = value + buf[i]
        return value

    to_members(gains_all, gain_s, gain_r)
    to_members(cnt_m, cnt_s, cnt_r)

    half = 2 if outer % 2 == 0 else 1
    hz = lax.rem(pz, half)
    hz_other = half - 1 - hz
    z_pair = (pz - hz + hz_other) * inner + px
    wrows = feats // (inner * half)

    def w_spot(c, j, x, h):
        return w_full.at[c, j, pl.ds(pl.multiple_of((x * half + h) * wrows, 16), wrows), :]

    @scoped
    def w_own(c):
        loads[c].wait()
        spot = w_spot(c, s, px, hz)
        for d in range(1, pairs):
            send(spot, spot, wy_s.at[c, d - 1], wy_r.at[c, d - 1], p, chip_at(d) * 2 + par)
        send(w_full.at[c, s], w_full.at[c, s], wt_s.at[c, 0], wt_r.at[c, 0], p, twin)

    def w_index(c, d):
        return c * (pairs - 1) + d - 1

    def w_sources():
        return [(d, chip_at(-d) * 2 + par) for d in range(1, pairs)]

    def w_to_x(spot, i, k):
        for e in range(1, inner):
            send(spot, spot, wx_s.at[i, e - 1, k], wx_r.at[i, e - 1, k], pz * inner + x_at(e), s)

    def w_to_z(spot, i, e):
        if half == 2:
            send(spot, spot, wz_s.at[i, e], wz_r.at[i, e], z_pair, s)

    def z_first(c):
        return c % 2 == 0

    @scoped
    def w_spread(c):
        for d, j in w_sources():
            i = w_index(c, d)
            spot = w_spot(c, j, px, hz)
            arrived(spot, wy_s.at[c, d - 1], wy_r.at[c, d - 1])
            w_to_z(spot, i, 0)
            w_to_x(spot, i, 0)

    @scoped
    def w_relay(c):
        for d, j in w_sources():
            i = w_index(c, d)
            if half == 1:
                continue
            if z_first(c):
                spot = w_spot(c, j, px, hz_other)
                arrived(spot, wz_s.at[i, 0], wz_r.at[i, 0])
                w_to_x(spot, i, 1)
            else:
                for e in range(1, inner):
                    spot = w_spot(c, j, x_at(-e), hz)
                    arrived(spot, wx_s.at[i, e - 1, 0], wx_r.at[i, e - 1, 0])
                    w_to_z(spot, i, e)

    @scoped
    def w_settle(c):
        for d, j in w_sources():
            i = w_index(c, d)
            if half == 1 or z_first(c):
                for k in range(half):
                    for e in range(1, inner):
                        h = hz_other if k else hz
                        arrived(w_spot(c, j, x_at(-e), h), wx_s.at[i, e - 1, k], wx_r.at[i, e - 1, k])
            else:
                for e in range(inner):
                    arrived(w_spot(c, j, x_at(-e), hz_other), wz_s.at[i, e], wz_r.at[i, e])
            send(w_full.at[c, j], w_full.at[c, j], wt_s.at[c, d], wt_r.at[c, d], p, twin)

    def w_ready(c):
        for d in range(pairs):
            j = chip_at(-d) * 2 + 1 - par
            arrived(w_full.at[c, j], wt_s.at[c, d], wt_r.at[c, d])

    for c in range(chunks):
        w_own(c)

    def part_of(e, b):
        return pl.ds(pl.multiple_of(x_at(e) * hrows + starts[b], 128), blocks[b])

    def n_index(d, h, b):
        return (((d - 1) * 2 + h) * len(blocks) + b) * inner

    with jax.named_scope("hidden"):
        loads[chunks].wait()
    step_rows = 32
    from_members(gains_all, gain_s, gain_r)

    def normalise(r, carry):
        rows = pl.ds(pl.multiple_of(r * step_rows, step_rows), step_rows)
        square = jnp.zeros((step_rows, 1), F32)
        for j in range(members):
            x = hidden[rows, pl.ds(j * feats, feats)].astype(F32)
            square = square + jnp.sum(x * x, axis=1, keepdims=True)
        inv = lax.rsqrt(square / width + EPSILON)
        for j in range(members):
            x = hidden[rows, pl.ds(j * feats, feats)].astype(F32)
            n_own[j, rows, :] = (x * inv * gains_all[j]).astype(BF16)
        return carry
    w_spread(0)
    with jax.named_scope("normalise"):
        lax.fori_loop(0, tokens // step_rows, normalise, 0)

    @scoped
    def n_send(b):
        for e in [*range(1, inner), 0]:
            for d in range(1, pairs):
                for h in range(2):
                    j = chip_at(d) * 2 + lax.rem(par + h, 2)
                    i = n_index(d, h, b) + e
                    send(n_own.at[j, :, part_of(e, b)], n_recv.at[s, :, part_of(e, b)], n_s.at[i], n_r.at[i], p, j)

    n_send(0)
    t_slot = (pairs - 1) * 2 * inner * len(blocks)
    send(n_own.at[twin], n_recv.at[s], n_s.at[t_slot], n_r.at[t_slot], p, twin)

    def turn(source, m, first, count):
        def step(b, carry):
            lanes = pl.ds(pl.multiple_of(first + b * 128, 128), 128)
            n_t[lanes, pl.ds(pl.multiple_of(m * tokens, 128), tokens)] = source[:, lanes].T
            return carry
        with jax.named_scope("turn"):
            lax.fori_loop(0, count // 128, step, 0)

    @scoped
    def n_land(b):
        for e in [*range(1, inner), 0]:
            for d in range(1, pairs):
                for h in range(2):
                    m = chip_at(-d) * 2 + lax.rem(par + h, 2)
                    i = n_index(d, h, b) + e
                    arrived(n_recv.at[m, :, part_of(e, b)], n_s.at[i], n_r.at[i])
                    turn(n_recv.at[m], m, x_at(e) * hrows + starts[b], blocks[b])

    @scoped
    def stage_keys(c, loss):
        w_ready(c)
        keys = jnp.dot(n_own[0], w_full[c, 0], preferred_element_type=F32)
        for j in range(1, members):
            keys = keys + jnp.dot(n_own[j], w_full[c, j], preferred_element_type=F32)
        diff = keys - teacher[:, lanes_of(c)].astype(F32)
        dk_all[c, s] = (scale * diff).astype(BF16)
        for d in range(1, pairs):
            send(
                dk_all.at[c, s], dk_all.at[c, s], dk_s.at[c, d - 1], dk_r.at[c, d - 1],
                p, chip_at(d) * 2 + par,
            )
        send(dk_all.at[c, s], dk_all.at[c, s], dks_s.at[c], dks_r.at[c], p, twin)
        return loss + jnp.sum(valid * diff * diff, axis=0, keepdims=True)

    @scoped
    def dk_pass(c):
        for d in range(1, pairs):
            q = chip_at(-d) * 2 + par
            arrived(dk_all.at[c, q], dk_s.at[c, d - 1], dk_r.at[c, d - 1])
            send(dk_all.at[c, q], dk_all.at[c, q], dkf_s.at[c, d - 1], dkf_r.at[c, d - 1], p, twin)

    def dk_ready(c):
        arrived(dk_all.at[c, twin], dks_s.at[c], dks_r.at[c])
        for d in range(1, pairs):
            q = chip_at(-d) * 2 + 1 - par
            arrived(dk_all.at[c, q], dkf_s.at[c, d - 1], dkf_r.at[c, d - 1])

    def product(b, c, e):
        dk = dk_all[c].reshape(members * tokens, kc)
        return jnp.dot(n_t[part_of(e, b), :], dk, preferred_element_type=F32)

    def unit_of(b, c):
        return b * chunks + c

    @scoped
    def stage_x(b, c):
        u, size = unit_of(b, c), blocks[b]
        for e in range(1, inner):
            src, dst = x_send.at[u, e - 1, pl.ds(0, size)], x_recv.at[u, e - 1, pl.ds(0, size)]
            x_send[u, e - 1, :size] = product(b, c, e).astype(BF16)
            send(src, dst, x_s.at[u, e - 1], x_r.at[u, e - 1], pz * inner + x_at(e), s)

    @scoped
    def stage_z(b, c):
        u, size = unit_of(b, c), blocks[b]
        q = size // outer
        grads[u, :size] = product(b, c, 0)
        for e in range(1, inner):
            arrived(x_recv.at[u, e - 1, pl.ds(0, size)], x_s.at[u, e - 1], x_r.at[u, e - 1])

        def sum_of(z):
            rows = pl.ds(pl.multiple_of(z * q, 16), q)
            value = grads[u, rows, :]
            for e in range(1, inner):
                value = value + x_recv[u, e - 1, rows, :].astype(F32)
            return value
        for k in range(1, outer):
            to = z_to(k)
            value = sum_of(to)
            if k == 1:
                z_near[u, :q] = value
                src, dst = z_near.at[u, pl.ds(0, q)], z_near_recv.at[u, pl.ds(0, q)]
            else:
                z_far[u, k - 2, :q] = value.astype(BF16)
                src, dst = z_far.at[u, k - 2, pl.ds(0, q)], z_far_recv.at[u, k - 2, pl.ds(0, q)]
            send(src, dst, z_s.at[u, k - 1], z_r.at[u, k - 1], to * inner + px, s)
        z_own[u, :q] = sum_of(pz)

    line = outer == 4
    far = 2 - 2 * (pz // 2)
    middle = (pz == 1) | (pz == 2)

    def out_spot(b, c, z):
        q = blocks[b] // outer
        return out.at[pl.ds(pl.multiple_of(px * hrows + starts[b] + z * q, 16), q), lanes_of(c)]

    def out_half(b, c, x):
        return out.at[pl.ds(pl.multiple_of(x * hrows + starts[b], 128), blocks[b]), lanes_of(c)]

    @scoped
    def stage_sum(b, c):
        u, q = unit_of(b, c), blocks[b] // outer
        value = z_own[u, :q]
        for k in range(1, outer):
            dst = z_near_recv.at[u, pl.ds(0, q)] if k == 1 else z_far_recv.at[u, k - 2, pl.ds(0, q)]
            arrived(dst, z_s.at[u, k - 1], z_r.at[u, k - 1])
            value = value + dst[...].astype(F32)
        spot = out_spot(b, c, pz)
        spot[...] = value.astype(BF16)
        if line:
            send(spot, spot, az_s.at[u, 0], az_r.at[u, 0], z_to(1) * inner + px, s)
            i = 1 + lax.rem(pz, 2)
            send(spot, spot, az_s.at[u, i], az_r.at[u, i], (2 - pz // 2) * inner + px, s)
        else:
            for k in range(1, outer):
                send(spot, spot, az_s.at[u, k - 1], az_r.at[u, k - 1], z_to(k) * inner + px, s)

    def far_copy(b, c):
        q = blocks[b] // outer
        first = px * hrows + starts[b] + far * q
        spot = out.at[pl.ds(pl.multiple_of(first, 16), 2 * q), lanes_of(c)]
        u = unit_of(b, c)
        return pltpu.make_async_remote_copy(
            src_ref=spot, dst_ref=spot, send_sem=af_s.at[u], recv_sem=af_r.at[u],
            device_id=(z_to(1) * inner + px, s), device_id_type=MESH,
        )

    @scoped
    def stage_far(b, c):
        if line:
            u = unit_of(b, c)

            @pl.when(middle)
            def _():
                for i in range(2):
                    arrived(out_spot(b, c, far + i), az_s.at[u, 1 + i], az_r.at[u, 1 + i])
                far_copy(b, c).start()

    @scoped
    def stage_relay(b, c):
        u = unit_of(b, c)
        if line:
            arrived(out_spot(b, c, z_to(1)), az_s.at[u, 0], az_r.at[u, 0])

            @pl.when(jnp.logical_not(middle))
            def _():
                far_copy(b, c).wait_recv()
        else:
            for k in range(1, outer):
                arrived(out_spot(b, c, z_from(k)), az_s.at[u, k - 1], az_r.at[u, k - 1])
        spot = out_half(b, c, px)
        for e in range(1, inner):
            send(spot, spot, ax_s.at[u, e - 1], ax_r.at[u, e - 1], pz * inner + x_at(e), s)

    @scoped
    def stage_settle(b, c):
        u = unit_of(b, c)
        for e in range(1, inner):
            arrived(out_half(b, c, x_at(-e)), ax_s.at[u, e - 1], ax_r.at[u, e - 1])

    turn(n_own.at[s], s, 0, feats)
    from_members(cnt_m, cnt_s, cnt_r)
    cnt_g[p] = total_of(cnt_m, members)
    to_groups(cnt_g, cntg_s, cntg_r)
    if chunks > 1:
        w_spread(1)
    w_relay(0)
    arrived(n_recv.at[twin], n_s.at[t_slot], n_r.at[t_slot])
    turn(n_recv.at[twin], twin, 0, feats)
    from_groups(cnt_g, cntg_s, cntg_r)
    total = total_of(cnt_g, groups)
    position = lax.broadcasted_iota(jnp.int32, (tokens, 1), 0)
    valid = jnp.where(position < rows_count * is_alive, 1.0, 0.0).astype(F32)
    scale = valid * (SCALE / total[:1, :1])

    loss = jnp.zeros((1, kc), F32)
    keyed, passed, landed = [0], [], []

    def next_keys(loss):
        c = keyed[0]
        if c + 2 < chunks:
            w_spread(c + 2)
        if c + 1 < chunks:
            w_relay(c + 1)
        w_settle(c)
        loss = stage_keys(c, loss)
        keyed[0] += 1
        if keyed[0] == chunks:
            loss_m[s] = jnp.broadcast_to(jnp.sum(loss, axis=1, keepdims=True), (8, 128))
            to_members(loss_m, loss_s, loss_r)
        return loss

    def ready(b, c):
        if b not in landed:
            landed.append(b)
            n_land(b)
        if c not in passed:
            passed.append(c)
            dk_pass(c)
            dk_ready(c)

    units = plan_of(len(blocks), chunks)
    def keys_and_columns(loss, count):
        while keyed[0] < count:
            loss = next_keys(loss)
            for b in range(1, len(blocks)):
                if min(AFTER_KEYS + b - 1, chunks) == keyed[0]:
                    n_send(b)
        return loss
    loss = keys_and_columns(loss, min(KEYS_AHEAD, chunks))
    stages = tuple(zip(LAGS, (stage_x, stage_z, stage_sum, stage_far, stage_relay)))
    if not X_FIRST:
        stages = stages[::-1]
    for i in range(len(units) + LAGS[-1]):
        if i == KEYS_STEP:
            loss = keys_and_columns(loss, chunks)
        for lag, stage in stages:
            if 0 <= i - lag < len(units) and units[i - lag]:
                if not lag:
                    ready(*units[i])
                stage(*units[i - lag])
        if i == len(units) - 1:
            from_members(loss_m, loss_s, loss_r)
            loss_g[p] = total_of(loss_m, members)
            to_groups(loss_g, lossg_s, lossg_r)
    from_groups(loss_g, lossg_s, lossg_r)
    loss_out[0, 0] = (total_of(loss_g, groups) / (2.0 * kv * total))[0, 0]
    for unit in units:
        if unit:
            stage_settle(*unit)
    with jax.named_scope("drain"):
        for copy in pending:
            copy.wait_send()
        if line:
            @pl.when(middle)
            def _():
                for b, c in filter(None, units):
                    far_copy(b, c).wait_send()


def body(members, groups, hidden_in, teacher, norm_gain, w_key, group_rows, member):
    tokens, width = hidden_in.shape
    owned, kv = w_key.shape
    inner = inner_of(groups)
    outer = groups // inner
    unit = math.lcm(128 * inner, 16 * groups)
    feats = -(-owned // unit) * unit
    blocks = blocks_of(feats // inner)
    units, most = len(blocks) * (kv // 256 if kv % 256 == 0 else 1), max(blocks)
    chunks = kv // 256 if kv % 256 == 0 else 1
    kc = kv // chunks
    gains = norm_gain.astype(F32)
    hidden, weights, wide_gains = hidden_in, w_key, norm_gain
    if feats != owned:
        extra = feats - owned
        hidden = jnp.pad(hidden_in.reshape(tokens, members, owned), ((0, 0), (0, 0), (0, extra)))
        hidden = hidden.reshape(tokens, members * feats)
        weights = jnp.pad(w_key, ((0, extra), (0, 0)))
        wide_gains = jnp.pad(norm_gain, (0, extra))
    pairs = members // 2
    vm = pltpu.VMEM

    def some(n):
        return max(n, 1)

    def sems(*shape):
        kind = pltpu.SemaphoreType.DMA(tuple(some(n) for n in shape))
        return [kind, kind]

    small = lambda n: vm((n, 8, 128), F32)
    space = pltpu.MemorySpace
    grad, loss = pl.pallas_call(
        functools.partial(kernel, members, groups, width, chunks, blocks),
        out_shape=(
            jax.ShapeDtypeStruct((feats, kv), BF16),
            jax.ShapeDtypeStruct((1, 1), F32),
        ),
        in_specs=[
            pl.BlockSpec(memory_space=pltpu.SMEM),
            pl.BlockSpec(memory_space=pltpu.SMEM),
            pl.BlockSpec(memory_space=pl.ANY),
            pl.BlockSpec(memory_space=pltpu.VMEM),
            pl.BlockSpec(memory_space=pltpu.VMEM),
            pl.BlockSpec(memory_space=pl.ANY),
        ],
        out_specs=(pl.BlockSpec(memory_space=pltpu.VMEM), pl.BlockSpec(memory_space=pltpu.SMEM)),
        scratch_shapes=[
            vm((tokens, members * feats), BF16),
            vm((chunks, members, feats, kc), BF16),
            vm((members, 1, feats), F32),
            small(members), small(groups), small(members), small(groups),
            vm((members, tokens, feats), BF16), vm((members, tokens, feats), BF16),
            vm((feats, members * tokens), BF16),
            vm((chunks, members, tokens, kc), BF16),
            vm((units, most, kc), F32),
            vm((units, some(inner - 1), most, kc), BF16), vm((units, some(inner - 1), most, kc), BF16),
            vm((units, most // outer, kc), F32), vm((units, most // outer, kc), F32),
            vm((units, some(outer - 2), most // outer, kc), BF16),
            vm((units, some(outer - 2), most // outer, kc), BF16),
            vm((units, most // outer, kc), F32),
            sems(chunks + 1)[0],
            *sems(members - 1), *sems(members - 1), *sems(groups - 1),
            *sems(members - 1), *sems(groups - 1),
            *sems(chunks, pairs - 1),
            *sems(chunks * (pairs - 1), inner), *sems(chunks * (pairs - 1), inner - 1, 2),
            *sems(chunks, pairs),
            *sems((pairs - 1) * 2 * inner * len(blocks) + 1),
            *sems(chunks, pairs - 1), *sems(chunks), *sems(chunks, pairs - 1),
            *sems(units, inner - 1), *sems(units, outer - 1),
            *sems(units, outer - 1), *sems(units), *sems(units, inner - 1),
        ],
        compiler_params=pltpu.CompilerParams(
            collective_id=0, has_side_effects=True, vmem_limit_bytes=60 * 1024 * 1024
        ),
    )(group_rows, member, hidden, teacher, wide_gains, weights)
    grad_key = grad[:owned].astype(F32)
    grad_gain = jnp.sum(grad_key * w_key.astype(F32), axis=1) / gains
    return (loss[0, 0], grad_gain, grad_key)


def solution(mesh):
    in_specs = (
        P(("dp", "shard"), None),
        P(("dp", "shard"), None),
        P("shard"),
        P("shard", None),
        P("dp"),
        P("dp", "shard"),
    )
    out_specs = (P(), P("shard"), P("shard", None))
    step = functools.partial(body, mesh.shape["shard"], mesh.shape["dp"])
    return jax.shard_map(step, mesh=mesh, in_specs=in_specs, out_specs=out_specs, check_vma=False)
```

```python
import functools
import math

import jax
import jax.numpy as jnp
from jax import lax
from jax.experimental import pallas as pl
from jax.experimental.pallas import tpu as pltpu
from jax.sharding import PartitionSpec as P

EPSILON = 1e-06
SCALE = 1024.0
MESH = pl.DeviceIdType.MESH
F32 = jnp.float32
BF16 = jnp.bfloat16


def inner_of(groups):
    return max(d for d in range(1, groups + 1) if groups % d == 0 and d * d <= groups)


def blocks_of(rows):
    unit = 128
    count = rows // unit
    if count == sum(SHARES):
        return [n * unit for n in SHARES]
    return [min(2, count - i) * unit for i in range(0, count, 2)]


SHARES, SEND_AFTER = (2, 1, 2), (0, 1, 3)
KEYS_AHEAD = 2
LAGS = (0, 2, 4, 6, 7)


def order_of(units):
    order = []
    for i in range(len(units) + LAGS[-1]):
        for lag, name in reversed(tuple(zip(LAGS, "XZSFR"))):
            if 0 <= i - lag < len(units):
                order.append((name, i - lag))
        if i == 0:
            order.append(("K", 0))
        if i == len(units) - 1:
            order.append(("L", 0))
    return order


def plan_of(blocks, chunks):
    return [(b, c) for c in range(chunks) for b in range(blocks)]


def paired(index, k, size):
    if size & (size - 1):
        return None
    out, bit = 0, 1
    while bit < size:
        out = out + lax.rem(lax.rem(index // bit, 2) + (k // bit) % 2, 2) * bit
        bit *= 2
    return out


def kernel(
    members, groups, width, chunks, blocks,
    live_rows, alive, hidden_in, teacher, gains, w_in,
    out, loss_out,
    hidden, w_full, gains_all, cnt_m, cnt_g, loss_m, loss_g,
    n_own, n_recv, n_t, dk_all, grads,
    x_send, x_recv, z_near, z_near_recv, z_far, z_far_recv, z_own,
    load_s, gain_s, gain_r, cnt_s, cnt_r, cntg_s, cntg_r,
    loss_s, loss_r, lossg_s, lossg_r, wy_s, wy_r, wz_s, wz_r, wx_s, wx_r, wt_s, wt_r,
    n_s, n_r, dk_s, dk_r, dks_s, dks_r, dkf_s, dkf_r,
    x_s, x_r, z_s, z_r, az_s, az_r, af_s, af_r, ax_s, ax_r,
):
    tokens, kv = teacher.shape
    feats = w_in.shape[0]
    kc = kv // chunks
    inner = inner_of(groups)
    outer = groups // inner
    hrows = feats // inner
    qrows = hrows // outer
    pairs = members // 2
    starts = [sum(blocks[:b]) for b in range(len(blocks))]
    p, s = lax.axis_index("dp"), lax.axis_index("shard")
    px, pz = lax.rem(p, inner), p // inner
    chip, par = s // 2, lax.rem(s, 2)
    twin = chip * 2 + 1 - par
    pending = []

    def scoped(stage):
        def run(c, *rest):
            with jax.named_scope("_".join([stage.__name__, str(c), *[str(r) for r in rest if isinstance(r, int)]])):
                return stage(c, *rest)
        return run

    def member_at(d):
        return lax.rem(s + d, members)

    def group_at(d):
        return lax.rem(p + d, groups)

    def chip_at(d):
        return lax.rem(chip + d + pairs, pairs)

    def x_at(d):
        return lax.rem(px + d + inner, inner)

    def z_to(k):
        q = paired(pz, k, outer)
        return lax.rem(pz + k, outer) if q is None else q

    def z_from(k):
        q = paired(pz, k, outer)
        return lax.rem(pz + outer - k, outer) if q is None else q

    def send(src, dst, ssem, rsem, group, member):
        copy = pltpu.make_async_remote_copy(
            src_ref=src, dst_ref=dst, send_sem=ssem, recv_sem=rsem,
            device_id=(group, member), device_id_type=MESH,
        )
        copy.start()
        pending.append(copy)

    def arrived(dst, ssem, rsem):
        pltpu.make_async_remote_copy(
            src_ref=dst, dst_ref=dst, send_sem=ssem, recv_sem=rsem,
            device_id=(p, twin), device_id_type=MESH,
        ).wait_recv()

    def lanes_of(c):
        return pl.ds(c * kc, kc)

    def rows_at(x, z):
        return pl.ds(pl.multiple_of(x * hrows + z * qrows, 16), qrows)

    loads = [
        pltpu.make_async_copy(w_in.at[:, lanes_of(c)], w_full.at[c, s], load_s.at[c])
        for c in range(chunks)
    ]
    loads.append(pltpu.make_async_copy(hidden_in, hidden, load_s.at[chunks]))
    for copy in loads:
        copy.start()

    rows_count, is_alive = live_rows[0], alive[0, 0]
    gains_all[s] = gains[...].astype(F32).reshape(1, feats)
    cnt_m[s] = jnp.broadcast_to((is_alive * rows_count).astype(F32), (8, 128))

    barrier = pltpu.get_barrier_semaphore()
    for d in range(1, members):
        pl.semaphore_signal(barrier, inc=1, device_id=(p, member_at(d)), device_id_type=MESH)
    for d in range(1, groups):
        pl.semaphore_signal(barrier, inc=1, device_id=(group_at(d), s), device_id_type=MESH)
    pl.semaphore_wait(barrier, members + groups - 2)

    def to_members(buf, ssem, rsem):
        for d in range(1, members):
            send(buf.at[s], buf.at[s], ssem.at[d - 1], rsem.at[d - 1], p, member_at(d))

    def from_members(buf, ssem, rsem):
        for d in range(1, members):
            j = lax.rem(s + members - d, members)
            arrived(buf.at[j], ssem.at[d - 1], rsem.at[d - 1])

    def to_groups(buf, ssem, rsem):
        for d in range(1, groups):
            send(buf.at[p], buf.at[p], ssem.at[d - 1], rsem.at[d - 1], group_at(d), s)

    def from_groups(buf, ssem, rsem):
        for d in range(1, groups):
            j = lax.rem(p + groups - d, groups)
            arrived(buf.at[j], ssem.at[d - 1], rsem.at[d - 1])

    def total_of(buf, n):
        value = buf[0]
        for i in range(1, n):
            value = value + buf[i]
        return value

    to_members(gains_all, gain_s, gain_r)
    to_members(cnt_m, cnt_s, cnt_r)

    half = 2 if outer % 2 == 0 else 1
    hz = lax.rem(pz, half)
    hz_other = half - 1 - hz
    z_pair = (pz - hz + hz_other) * inner + px
    wrows = feats // (inner * half)

    def w_spot(c, j, x, h):
        return w_full.at[c, j, pl.ds(pl.multiple_of((x * half + h) * wrows, 16), wrows), :]

    @scoped
    def w_own(c):
        loads[c].wait()
        spot = w_spot(c, s, px, hz)
        for d in range(1, pairs):
            send(spot, spot, wy_s.at[c, d - 1], wy_r.at[c, d - 1], p, chip_at(d) * 2 + par)
        send(w_full.at[c, s], w_full.at[c, s], wt_s.at[c, 0], wt_r.at[c, 0], p, twin)

    def w_index(c, d):
        return c * (pairs - 1) + d - 1

    def w_sources():
        return [(d, chip_at(-d) * 2 + par) for d in range(1, pairs)]

    def w_to_x(spot, i, k):
        for e in range(1, inner):
            send(spot, spot, wx_s.at[i, e - 1, k], wx_r.at[i, e - 1, k], pz * inner + x_at(e), s)

    def w_to_z(spot, i, e):
        if half == 2:
            send(spot, spot, wz_s.at[i, e], wz_r.at[i, e], z_pair, s)

    def z_first(c):
        return c % 2 == 0

    @scoped
    def w_spread(c):
        for d, j in w_sources():
            i = w_index(c, d)
            spot = w_spot(c, j, px, hz)
            arrived(spot, wy_s.at[c, d - 1], wy_r.at[c, d - 1])
            w_to_z(spot, i, 0)
            w_to_x(spot, i, 0)

    @scoped
    def w_relay(c):
        for d, j in w_sources():
            i = w_index(c, d)
            if half == 1:
                continue
            if z_first(c):
                spot = w_spot(c, j, px, hz_other)
                arrived(spot, wz_s.at[i, 0], wz_r.at[i, 0])
                w_to_x(spot, i, 1)
            else:
                for e in range(1, inner):
                    spot = w_spot(c, j, x_at(-e), hz)
                    arrived(spot, wx_s.at[i, e - 1, 0], wx_r.at[i, e - 1, 0])
                    w_to_z(spot, i, e)

    @scoped
    def w_settle(c):
        for d, j in w_sources():
            i = w_index(c, d)
            if half == 1 or z_first(c):
                for k in range(half):
                    for e in range(1, inner):
                        h = hz_other if k else hz
                        arrived(w_spot(c, j, x_at(-e), h), wx_s.at[i, e - 1, k], wx_r.at[i, e - 1, k])
            else:
                for e in range(inner):
                    arrived(w_spot(c, j, x_at(-e), hz_other), wz_s.at[i, e], wz_r.at[i, e])
            send(w_full.at[c, j], w_full.at[c, j], wt_s.at[c, d], wt_r.at[c, d], p, twin)

    def w_ready(c):
        for d in range(pairs):
            j = chip_at(-d) * 2 + 1 - par
            arrived(w_full.at[c, j], wt_s.at[c, d], wt_r.at[c, d])

    for c in range(chunks):
        w_own(c)

    def part_of(e, b):
        return pl.ds(pl.multiple_of(x_at(e) * hrows + starts[b], 128), blocks[b])

    def n_index(d, h, b):
        return (((d - 1) * 2 + h) * len(blocks) + b) * inner

    with jax.named_scope("hidden"):
        loads[chunks].wait()
    step_rows = 32
    from_members(gains_all, gain_s, gain_r)

    def normalise(r, carry):
        rows = pl.ds(pl.multiple_of(r * step_rows, step_rows), step_rows)
        square = jnp.zeros((step_rows, 1), F32)
        for j in range(members):
            x = hidden[rows, pl.ds(j * feats, feats)].astype(F32)
            square = square + jnp.sum(x * x, axis=1, keepdims=True)
        inv = lax.rsqrt(square / width + EPSILON)
        for j in range(members):
            x = hidden[rows, pl.ds(j * feats, feats)].astype(F32)
            n_own[j, rows, :] = (x * inv * gains_all[j]).astype(BF16)
        return carry
    w_spread(0)
    with jax.named_scope("normalise"):
        lax.fori_loop(0, tokens // step_rows, normalise, 0)

    @scoped
    def n_send(b):
        for e in [*range(1, inner), 0]:
            for d in range(1, pairs):
                for h in range(2):
                    j = chip_at(d) * 2 + lax.rem(par + h, 2)
                    i = n_index(d, h, b) + e
                    send(n_own.at[j, :, part_of(e, b)], n_recv.at[s, :, part_of(e, b)], n_s.at[i], n_r.at[i], p, j)

    n_send(0)
    t_slot = (pairs - 1) * 2 * inner * len(blocks)
    send(n_own.at[twin], n_recv.at[s], n_s.at[t_slot], n_r.at[t_slot], p, twin)

    def turn(source, m, first, count):
        def step(b, carry):
            lanes = pl.ds(pl.multiple_of(first + b * 128, 128), 128)
            n_t[lanes, pl.ds(pl.multiple_of(m * tokens, 128), tokens)] = source[:, lanes].T
            return carry
        with jax.named_scope("turn"):
            lax.fori_loop(0, count // 128, step, 0)

    @scoped
    def n_land(b):
        for e in [*range(1, inner), 0]:
            for d in range(1, pairs):
                for h in range(2):
                    m = chip_at(-d) * 2 + lax.rem(par + h, 2)
                    i = n_index(d, h, b) + e
                    arrived(n_recv.at[m, :, part_of(e, b)], n_s.at[i], n_r.at[i])
                    turn(n_recv.at[m], m, x_at(e) * hrows + starts[b], blocks[b])

    @scoped
    def stage_keys(c, loss):
        w_ready(c)
        keys = jnp.dot(n_own[0], w_full[c, 0], preferred_element_type=F32)
        for j in range(1, members):
            keys = keys + jnp.dot(n_own[j], w_full[c, j], preferred_element_type=F32)
        diff = keys - teacher[:, lanes_of(c)].astype(F32)
        dk_all[c, s] = (scale * diff).astype(BF16)
        for d in range(1, pairs):
            send(
                dk_all.at[c, s], dk_all.at[c, s], dk_s.at[c, d - 1], dk_r.at[c, d - 1],
                p, chip_at(d) * 2 + par,
            )
        send(dk_all.at[c, s], dk_all.at[c, s], dks_s.at[c], dks_r.at[c], p, twin)
        return loss + jnp.sum(valid * diff * diff, axis=0, keepdims=True)

    @scoped
    def dk_pass(c):
        for d in range(1, pairs):
            q = chip_at(-d) * 2 + par
            arrived(dk_all.at[c, q], dk_s.at[c, d - 1], dk_r.at[c, d - 1])
            send(dk_all.at[c, q], dk_all.at[c, q], dkf_s.at[c, d - 1], dkf_r.at[c, d - 1], p, twin)

    def dk_ready(c):
        arrived(dk_all.at[c, twin], dks_s.at[c], dks_r.at[c])
        for d in range(1, pairs):
            q = chip_at(-d) * 2 + 1 - par
            arrived(dk_all.at[c, q], dkf_s.at[c, d - 1], dkf_r.at[c, d - 1])

    def product(b, c, e):
        dk = dk_all[c].reshape(members * tokens, kc)
        return jnp.dot(n_t[part_of(e, b), :], dk, preferred_element_type=F32)

    def unit_of(b, c):
        return b * chunks + c

    @scoped
    def stage_x(b, c):
        u, size = unit_of(b, c), blocks[b]
        for e in range(1, inner):
            src, dst = x_send.at[u, e - 1, pl.ds(0, size)], x_recv.at[u, e - 1, pl.ds(0, size)]
            x_send[u, e - 1, :size] = product(b, c, e).astype(BF16)
            send(src, dst, x_s.at[u, e - 1], x_r.at[u, e - 1], pz * inner + x_at(e), s)

    @scoped
    def stage_z(b, c):
        u, size = unit_of(b, c), blocks[b]
        q = size // outer
        grads[u, :size] = product(b, c, 0)
        for e in range(1, inner):
            arrived(x_recv.at[u, e - 1, pl.ds(0, size)], x_s.at[u, e - 1], x_r.at[u, e - 1])

        def sum_of(z):
            rows = pl.ds(pl.multiple_of(z * q, 16), q)
            value = grads[u, rows, :]
            for e in range(1, inner):
                value = value + x_recv[u, e - 1, rows, :].astype(F32)
            return value
        for k in range(1, outer):
            to = z_to(k)
            value = sum_of(to)
            if k == 1:
                z_near[u, :q] = value
                src, dst = z_near.at[u, pl.ds(0, q)], z_near_recv.at[u, pl.ds(0, q)]
            else:
                z_far[u, k - 2, :q] = value.astype(BF16)
                src, dst = z_far.at[u, k - 2, pl.ds(0, q)], z_far_recv.at[u, k - 2, pl.ds(0, q)]
            send(src, dst, z_s.at[u, k - 1], z_r.at[u, k - 1], to * inner + px, s)
        z_own[u, :q] = sum_of(pz)

    line = outer == 4
    far = 2 - 2 * (pz // 2)
    middle = (pz == 1) | (pz == 2)

    def out_spot(b, c, z):
        q = blocks[b] // outer
        return out.at[pl.ds(pl.multiple_of(px * hrows + starts[b] + z * q, 16), q), lanes_of(c)]

    def out_half(b, c, x):
        return out.at[pl.ds(pl.multiple_of(x * hrows + starts[b], 128), blocks[b]), lanes_of(c)]

    @scoped
    def stage_sum(b, c):
        u, q = unit_of(b, c), blocks[b] // outer
        value = z_own[u, :q]
        for k in range(1, outer):
            dst = z_near_recv.at[u, pl.ds(0, q)] if k == 1 else z_far_recv.at[u, k - 2, pl.ds(0, q)]
            arrived(dst, z_s.at[u, k - 1], z_r.at[u, k - 1])
            value = value + dst[...].astype(F32)
        spot = out_spot(b, c, pz)
        spot[...] = value.astype(BF16)
        if line:
            send(spot, spot, az_s.at[u, 0], az_r.at[u, 0], z_to(1) * inner + px, s)
            i = 1 + lax.rem(pz, 2)
            send(spot, spot, az_s.at[u, i], az_r.at[u, i], (2 - pz // 2) * inner + px, s)
        else:
            for k in range(1, outer):
                send(spot, spot, az_s.at[u, k - 1], az_r.at[u, k - 1], z_to(k) * inner + px, s)

    def far_copy(b, c):
        q = blocks[b] // outer
        first = px * hrows + starts[b] + far * q
        spot = out.at[pl.ds(pl.multiple_of(first, 16), 2 * q), lanes_of(c)]
        u = unit_of(b, c)
        return pltpu.make_async_remote_copy(
            src_ref=spot, dst_ref=spot, send_sem=af_s.at[u], recv_sem=af_r.at[u],
            device_id=(z_to(1) * inner + px, s), device_id_type=MESH,
        )

    @scoped
    def stage_far(b, c):
        if line:
            u = unit_of(b, c)

            @pl.when(middle)
            def _():
                for i in range(2):
                    arrived(out_spot(b, c, far + i), az_s.at[u, 1 + i], az_r.at[u, 1 + i])
                far_copy(b, c).start()

    @scoped
    def stage_relay(b, c):
        u = unit_of(b, c)
        if line:
            arrived(out_spot(b, c, z_to(1)), az_s.at[u, 0], az_r.at[u, 0])

            @pl.when(jnp.logical_not(middle))
            def _():
                far_copy(b, c).wait_recv()
        else:
            for k in range(1, outer):
                arrived(out_spot(b, c, z_from(k)), az_s.at[u, k - 1], az_r.at[u, k - 1])
        spot = out_half(b, c, px)
        for e in range(1, inner):
            send(spot, spot, ax_s.at[u, e - 1], ax_r.at[u, e - 1], pz * inner + x_at(e), s)

    @scoped
    def stage_settle(b, c):
        u = unit_of(b, c)
        for e in range(1, inner):
            arrived(out_half(b, c, x_at(-e)), ax_s.at[u, e - 1], ax_r.at[u, e - 1])

    turn(n_own.at[s], s, 0, feats)
    from_members(cnt_m, cnt_s, cnt_r)
    cnt_g[p] = total_of(cnt_m, members)
    to_groups(cnt_g, cntg_s, cntg_r)
    if chunks > 1:
        w_spread(1)
    w_relay(0)
    arrived(n_recv.at[twin], n_s.at[t_slot], n_r.at[t_slot])
    turn(n_recv.at[twin], twin, 0, feats)
    from_groups(cnt_g, cntg_s, cntg_r)
    total = total_of(cnt_g, groups)
    position = lax.broadcasted_iota(jnp.int32, (tokens, 1), 0)
    valid = jnp.where(position < rows_count * is_alive, 1.0, 0.0).astype(F32)
    scale = valid * (SCALE / total[:1, :1])

    loss = jnp.zeros((1, kc), F32)
    keyed, passed, landed = [0], [], []

    def next_keys(loss):
        c = keyed[0]
        if c + 2 < chunks:
            w_spread(c + 2)
        if c + 1 < chunks:
            w_relay(c + 1)
        w_settle(c)
        loss = stage_keys(c, loss)
        keyed[0] += 1
        if keyed[0] == chunks:
            loss_m[s] = jnp.broadcast_to(jnp.sum(loss, axis=1, keepdims=True), (8, 128))
            to_members(loss_m, loss_s, loss_r)
        return loss

    def ready(b, c):
        if b not in landed:
            landed.append(b)
            n_land(b)
        if c not in passed:
            passed.append(c)
            dk_pass(c)
            dk_ready(c)

    units = plan_of(len(blocks), chunks)
    def keys_and_columns(loss, count):
        while keyed[0] < count:
            loss = next_keys(loss)
            for b in range(1, len(blocks)):
                if min(SEND_AFTER[min(b, 2)], chunks) == keyed[0]:
                    n_send(b)
        return loss
    loss = keys_and_columns(loss, min(KEYS_AHEAD, chunks))
    stages = {"X": stage_x, "Z": stage_z, "S": stage_sum, "F": stage_far, "R": stage_relay}
    for name, i in order_of(units):
        if name == "K":
            loss = keys_and_columns(loss, chunks)
        elif name == "L":
            from_members(loss_m, loss_s, loss_r)
            loss_g[p] = total_of(loss_m, members)
            to_groups(loss_g, lossg_s, lossg_r)
        else:
            if name == "X":
                ready(*units[i])
            stages[name](*units[i])
    from_groups(loss_g, lossg_s, lossg_r)
    loss_out[0, 0] = (total_of(loss_g, groups) / (2.0 * kv * total))[0, 0]
    for unit in units:
        if unit:
            stage_settle(*unit)
    with jax.named_scope("drain"):
        for copy in pending:
            copy.wait_send()
        if line:
            @pl.when(middle)
            def _():
                for b, c in filter(None, units):
                    far_copy(b, c).wait_send()


def body(members, groups, hidden_in, teacher, norm_gain, w_key, group_rows, member):
    tokens, width = hidden_in.shape
    owned, kv = w_key.shape
    inner = inner_of(groups)
    outer = groups // inner
    unit = math.lcm(128 * inner, 16 * groups)
    feats = -(-owned // unit) * unit
    blocks = blocks_of(feats // inner)
    units, most = len(blocks) * (kv // 256 if kv % 256 == 0 else 1), max(blocks)
    chunks = kv // 256 if kv % 256 == 0 else 1
    kc = kv // chunks
    gains = norm_gain.astype(F32)
    hidden, weights, wide_gains = hidden_in, w_key, norm_gain
    if feats != owned:
        extra = feats - owned
        hidden = jnp.pad(hidden_in.reshape(tokens, members, owned), ((0, 0), (0, 0), (0, extra)))
        hidden = hidden.reshape(tokens, members * feats)
        weights = jnp.pad(w_key, ((0, extra), (0, 0)))
        wide_gains = jnp.pad(norm_gain, (0, extra))
    pairs = members // 2
    vm = pltpu.VMEM

    def some(n):
        return max(n, 1)

    def sems(*shape):
        kind = pltpu.SemaphoreType.DMA(tuple(some(n) for n in shape))
        return [kind, kind]

    small = lambda n: vm((n, 8, 128), F32)
    space = pltpu.MemorySpace
    grad, loss = pl.pallas_call(
        functools.partial(kernel, members, groups, width, chunks, blocks),
        out_shape=(
            jax.ShapeDtypeStruct((feats, kv), BF16),
            jax.ShapeDtypeStruct((1, 1), F32),
        ),
        in_specs=[
            pl.BlockSpec(memory_space=pltpu.SMEM),
            pl.BlockSpec(memory_space=pltpu.SMEM),
            pl.BlockSpec(memory_space=pl.ANY),
            pl.BlockSpec(memory_space=pltpu.VMEM),
            pl.BlockSpec(memory_space=pltpu.VMEM),
            pl.BlockSpec(memory_space=pl.ANY),
        ],
        out_specs=(pl.BlockSpec(memory_space=pltpu.VMEM), pl.BlockSpec(memory_space=pltpu.SMEM)),
        scratch_shapes=[
            vm((tokens, members * feats), BF16),
            vm((chunks, members, feats, kc), BF16),
            vm((members, 1, feats), F32),
            small(members), small(groups), small(members), small(groups),
            vm((members, tokens, feats), BF16), vm((members, tokens, feats), BF16),
            vm((feats, members * tokens), BF16),
            vm((chunks, members, tokens, kc), BF16),
            vm((units, most, kc), F32),
            vm((units, some(inner - 1), most, kc), BF16), vm((units, some(inner - 1), most, kc), BF16),
            vm((units, most // outer, kc), F32), vm((units, most // outer, kc), F32),
            vm((units, some(outer - 2), most // outer, kc), BF16),
            vm((units, some(outer - 2), most // outer, kc), BF16),
            vm((units, most // outer, kc), F32),
            sems(chunks + 1)[0],
            *sems(members - 1), *sems(members - 1), *sems(groups - 1),
            *sems(members - 1), *sems(groups - 1),
            *sems(chunks, pairs - 1),
            *sems(chunks * (pairs - 1), inner), *sems(chunks * (pairs - 1), inner - 1, 2),
            *sems(chunks, pairs),
            *sems((pairs - 1) * 2 * inner * len(blocks) + 1),
            *sems(chunks, pairs - 1), *sems(chunks), *sems(chunks, pairs - 1),
            *sems(units, inner - 1), *sems(units, outer - 1),
            *sems(units, outer - 1), *sems(units), *sems(units, inner - 1),
        ],
        compiler_params=pltpu.CompilerParams(
            collective_id=0, has_side_effects=True, vmem_limit_bytes=60 * 1024 * 1024
        ),
    )(group_rows, member, hidden, teacher, wide_gains, weights)
    grad_key = grad[:owned].astype(F32)
    grad_gain = jnp.sum(grad_key * w_key.astype(F32), axis=1) / gains
    return (loss[0, 0], grad_gain, grad_key)


def solution(mesh):
    in_specs = (
        P(("dp", "shard"), None),
        P(("dp", "shard"), None),
        P("shard"),
        P("shard", None),
        P("dp"),
        P("dp", "shard"),
    )
    out_specs = (P(), P("shard"), P("shard", None))
    step = functools.partial(body, mesh.shape["shard"], mesh.shape["dp"])
    return jax.shard_map(step, mesh=mesh, in_specs=in_specs, out_specs=out_specs, check_vma=False)
```

```python
import functools
import math

import jax
import jax.numpy as jnp
from jax import lax
from jax.experimental import pallas as pl
from jax.experimental.pallas import tpu as pltpu
from jax.sharding import PartitionSpec as P

EPSILON = 1e-06
SCALE = 1024.0
MESH = pl.DeviceIdType.MESH
F32 = jnp.float32
BF16 = jnp.bfloat16


def inner_of(groups):
    return max(d for d in range(1, groups + 1) if groups % d == 0 and d * d <= groups)


def blocks_of(rows):
    unit = 128
    count = rows // unit
    if count == sum(SHARES):
        return [n * unit for n in SHARES]
    return [min(2, count - i) * unit for i in range(0, count, 2)]


SHARES, SEND_AFTER = (2, 1, 2), (0, 1, 3)
KEYS_AHEAD = 2
LAGS = (0, 2, 4, 6, 7)


def order_of(units):
    order = []
    for i in range(len(units) + LAGS[-1]):
        for lag, name in reversed(tuple(zip(LAGS, "XZSFR"))):
            if 0 <= i - lag < len(units):
                order.append((name, i - lag))
        if i == 0:
            order.append(("K", 0))
        if i == len(units) - 1:
            order.append(("L", 0))
    return order


def plan_of(blocks, chunks):
    early = max(blocks - 1, 1)
    first = [(b, c) for c in range(chunks) for b in range(early)]
    return first + [(b, c) for b in range(early, blocks) for c in range(chunks)]


def paired(index, k, size):
    if size & (size - 1):
        return None
    out, bit = 0, 1
    while bit < size:
        out = out + lax.rem(lax.rem(index // bit, 2) + (k // bit) % 2, 2) * bit
        bit *= 2
    return out


def kernel(
    members, groups, width, chunks, blocks,
    live_rows, alive, hidden_in, teacher, gains, w_in,
    out, loss_out,
    hidden, w_full, gains_all, cnt_m, cnt_g, loss_m, loss_g,
    n_own, n_recv, n_t, dk_all, grads,
    x_send, x_recv, z_near, z_near_recv, z_far, z_far_recv, z_own,
    load_s, gain_s, gain_r, cnt_s, cnt_r, cntg_s, cntg_r,
    loss_s, loss_r, lossg_s, lossg_r, wy_s, wy_r, wz_s, wz_r, wx_s, wx_r, wt_s, wt_r,
    n_s, n_r, dk_s, dk_r, dks_s, dks_r, dkf_s, dkf_r,
    x_s, x_r, z_s, z_r, az_s, az_r, af_s, af_r, ax_s, ax_r,
):
    tokens, kv = teacher.shape
    feats = w_in.shape[0]
    kc = kv // chunks
    inner = inner_of(groups)
    outer = groups // inner
    hrows = feats // inner
    qrows = hrows // outer
    pairs = members // 2
    starts = [sum(blocks[:b]) for b in range(len(blocks))]
    p, s = lax.axis_index("dp"), lax.axis_index("shard")
    px, pz = lax.rem(p, inner), p // inner
    chip, par = s // 2, lax.rem(s, 2)
    twin = chip * 2 + 1 - par
    pending = []

    def scoped(stage):
        def run(c, *rest):
            with jax.named_scope("_".join([stage.__name__, str(c), *[str(r) for r in rest if isinstance(r, int)]])):
                return stage(c, *rest)
        return run

    def member_at(d):
        return lax.rem(s + d, members)

    def group_at(d):
        return lax.rem(p + d, groups)

    def chip_at(d):
        return lax.rem(chip + d + pairs, pairs)

    def x_at(d):
        return lax.rem(px + d + inner, inner)

    def z_to(k):
        q = paired(pz, k, outer)
        return lax.rem(pz + k, outer) if q is None else q

    def z_from(k):
        q = paired(pz, k, outer)
        return lax.rem(pz + outer - k, outer) if q is None else q

    def send(src, dst, ssem, rsem, group, member):
        copy = pltpu.make_async_remote_copy(
            src_ref=src, dst_ref=dst, send_sem=ssem, recv_sem=rsem,
            device_id=(group, member), device_id_type=MESH,
        )
        copy.start()
        pending.append(copy)

    def arrived(dst, ssem, rsem):
        pltpu.make_async_remote_copy(
            src_ref=dst, dst_ref=dst, send_sem=ssem, recv_sem=rsem,
            device_id=(p, twin), device_id_type=MESH,
        ).wait_recv()

    def lanes_of(c):
        return pl.ds(c * kc, kc)

    def rows_at(x, z):
        return pl.ds(pl.multiple_of(x * hrows + z * qrows, 16), qrows)

    loads = [
        pltpu.make_async_copy(w_in.at[:, lanes_of(c)], w_full.at[c, s], load_s.at[c])
        for c in range(chunks)
    ]
    loads.append(pltpu.make_async_copy(hidden_in, hidden, load_s.at[chunks]))
    for copy in loads:
        copy.start()

    rows_count, is_alive = live_rows[0], alive[0, 0]
    gains_all[s] = gains[...].astype(F32).reshape(1, feats)
    cnt_m[s] = jnp.broadcast_to((is_alive * rows_count).astype(F32), (8, 128))

    barrier = pltpu.get_barrier_semaphore()
    for d in range(1, members):
        pl.semaphore_signal(barrier, inc=1, device_id=(p, member_at(d)), device_id_type=MESH)
    for d in range(1, groups):
        pl.semaphore_signal(barrier, inc=1, device_id=(group_at(d), s), device_id_type=MESH)
    pl.semaphore_wait(barrier, members + groups - 2)

    def to_members(buf, ssem, rsem):
        for d in range(1, members):
            send(buf.at[s], buf.at[s], ssem.at[d - 1], rsem.at[d - 1], p, member_at(d))

    def from_members(buf, ssem, rsem):
        for d in range(1, members):
            j = lax.rem(s + members - d, members)
            arrived(buf.at[j], ssem.at[d - 1], rsem.at[d - 1])

    def to_groups(buf, ssem, rsem):
        for d in range(1, groups):
            send(buf.at[p], buf.at[p], ssem.at[d - 1], rsem.at[d - 1], group_at(d), s)

    def from_groups(buf, ssem, rsem):
        for d in range(1, groups):
            j = lax.rem(p + groups - d, groups)
            arrived(buf.at[j], ssem.at[d - 1], rsem.at[d - 1])

    def total_of(buf, n):
        value = buf[0]
        for i in range(1, n):
            value = value + buf[i]
        return value

    to_members(gains_all, gain_s, gain_r)
    to_members(cnt_m, cnt_s, cnt_r)

    half = 2 if outer % 2 == 0 else 1
    hz = lax.rem(pz, half)
    hz_other = half - 1 - hz
    z_pair = (pz - hz + hz_other) * inner + px
    wrows = feats // (inner * half)

    def w_spot(c, j, x, h):
        return w_full.at[c, j, pl.ds(pl.multiple_of((x * half + h) * wrows, 16), wrows), :]

    @scoped
    def w_own(c):
        loads[c].wait()
        spot = w_spot(c, s, px, hz)
        for d in range(1, pairs):
            send(spot, spot, wy_s.at[c, d - 1], wy_r.at[c, d - 1], p, chip_at(d) * 2 + par)
        send(w_full.at[c, s], w_full.at[c, s], wt_s.at[c, 0], wt_r.at[c, 0], p, twin)

    def w_index(c, d):
        return c * (pairs - 1) + d - 1

    def w_sources():
        return [(d, chip_at(-d) * 2 + par) for d in range(1, pairs)]

    def w_to_x(spot, i, k):
        for e in range(1, inner):
            send(spot, spot, wx_s.at[i, e - 1, k], wx_r.at[i, e - 1, k], pz * inner + x_at(e), s)

    def w_to_z(spot, i, e):
        if half == 2:
            send(spot, spot, wz_s.at[i, e], wz_r.at[i, e], z_pair, s)

    def z_first(c):
        return c % 2 == 0

    @scoped
    def w_spread(c):
        for d, j in w_sources():
            i = w_index(c, d)
            spot = w_spot(c, j, px, hz)
            arrived(spot, wy_s.at[c, d - 1], wy_r.at[c, d - 1])
            w_to_z(spot, i, 0)
            w_to_x(spot, i, 0)

    @scoped
    def w_relay(c):
        for d, j in w_sources():
            i = w_index(c, d)
            if half == 1:
                continue
            if z_first(c):
                spot = w_spot(c, j, px, hz_other)
                arrived(spot, wz_s.at[i, 0], wz_r.at[i, 0])
                w_to_x(spot, i, 1)
            else:
                for e in range(1, inner):
                    spot = w_spot(c, j, x_at(-e), hz)
                    arrived(spot, wx_s.at[i, e - 1, 0], wx_r.at[i, e - 1, 0])
                    w_to_z(spot, i, e)

    @scoped
    def w_settle(c):
        for d, j in w_sources():
            i = w_index(c, d)
            if half == 1 or z_first(c):
                for k in range(half):
                    for e in range(1, inner):
                        h = hz_other if k else hz
                        arrived(w_spot(c, j, x_at(-e), h), wx_s.at[i, e - 1, k], wx_r.at[i, e - 1, k])
            else:
                for e in range(inner):
                    arrived(w_spot(c, j, x_at(-e), hz_other), wz_s.at[i, e], wz_r.at[i, e])
            send(w_full.at[c, j], w_full.at[c, j], wt_s.at[c, d], wt_r.at[c, d], p, twin)

    def w_ready(c):
        for d in range(pairs):
            j = chip_at(-d) * 2 + 1 - par
            arrived(w_full.at[c, j], wt_s.at[c, d], wt_r.at[c, d])

    for c in range(chunks):
        w_own(c)

    def part_of(e, b):
        return pl.ds(pl.multiple_of(x_at(e) * hrows + starts[b], 128), blocks[b])

    def n_index(d, h, b):
        return (((d - 1) * 2 + h) * len(blocks) + b) * inner

    with jax.named_scope("hidden"):
        loads[chunks].wait()
    step_rows = 32
    from_members(gains_all, gain_s, gain_r)

    def normalise(r, carry):
        rows = pl.ds(pl.multiple_of(r * step_rows, step_rows), step_rows)
        square = jnp.zeros((step_rows, 1), F32)
        for j in range(members):
            x = hidden[rows, pl.ds(j * feats, feats)].astype(F32)
            square = square + jnp.sum(x * x, axis=1, keepdims=True)
        inv = lax.rsqrt(square / width + EPSILON)
        for j in range(members):
            x = hidden[rows, pl.ds(j * feats, feats)].astype(F32)
            n_own[j, rows, :] = (x * inv * gains_all[j]).astype(BF16)
        return carry
    w_spread(0)
    with jax.named_scope("normalise"):
        lax.fori_loop(0, tokens // step_rows, normalise, 0)

    @scoped
    def n_send(b):
        for e in [*range(1, inner), 0]:
            for d in range(1, pairs):
                for h in range(2):
                    j = chip_at(d) * 2 + lax.rem(par + h, 2)
                    i = n_index(d, h, b) + e
                    send(n_own.at[j, :, part_of(e, b)], n_recv.at[s, :, part_of(e, b)], n_s.at[i], n_r.at[i], p, j)

    n_send(0)
    t_slot = (pairs - 1) * 2 * inner * len(blocks)
    send(n_own.at[twin], n_recv.at[s], n_s.at[t_slot], n_r.at[t_slot], p, twin)

    def turn(source, m, first, count):
        def step(b, carry):
            lanes = pl.ds(pl.multiple_of(first + b * 128, 128), 128)
            n_t[lanes, pl.ds(pl.multiple_of(m * tokens, 128), tokens)] = source[:, lanes].T
            return carry
        with jax.named_scope("turn"):
            lax.fori_loop(0, count // 128, step, 0)

    @scoped
    def n_land(b):
        for e in [*range(1, inner), 0]:
            for d in range(1, pairs):
                for h in range(2):
                    m = chip_at(-d) * 2 + lax.rem(par + h, 2)
                    i = n_index(d, h, b) + e
                    arrived(n_recv.at[m, :, part_of(e, b)], n_s.at[i], n_r.at[i])
                    turn(n_recv.at[m], m, x_at(e) * hrows + starts[b], blocks[b])

    @scoped
    def stage_keys(c, loss):
        w_ready(c)
        keys = jnp.dot(n_own[0], w_full[c, 0], preferred_element_type=F32)
        for j in range(1, members):
            keys = keys + jnp.dot(n_own[j], w_full[c, j], preferred_element_type=F32)
        diff = keys - teacher[:, lanes_of(c)].astype(F32)
        dk_all[c, s] = (scale * diff).astype(BF16)
        for d in range(1, pairs):
            send(
                dk_all.at[c, s], dk_all.at[c, s], dk_s.at[c, d - 1], dk_r.at[c, d - 1],
                p, chip_at(d) * 2 + par,
            )
        send(dk_all.at[c, s], dk_all.at[c, s], dks_s.at[c], dks_r.at[c], p, twin)
        return loss + jnp.sum(valid * diff * diff, axis=0, keepdims=True)

    @scoped
    def dk_pass(c):
        for d in range(1, pairs):
            q = chip_at(-d) * 2 + par
            arrived(dk_all.at[c, q], dk_s.at[c, d - 1], dk_r.at[c, d - 1])
            send(dk_all.at[c, q], dk_all.at[c, q], dkf_s.at[c, d - 1], dkf_r.at[c, d - 1], p, twin)

    def dk_ready(c):
        arrived(dk_all.at[c, twin], dks_s.at[c], dks_r.at[c])
        for d in range(1, pairs):
            q = chip_at(-d) * 2 + 1 - par
            arrived(dk_all.at[c, q], dkf_s.at[c, d - 1], dkf_r.at[c, d - 1])

    def product(b, c, e):
        dk = dk_all[c].reshape(members * tokens, kc)
        return jnp.dot(n_t[part_of(e, b), :], dk, preferred_element_type=F32)

    def unit_of(b, c):
        return b * chunks + c

    @scoped
    def stage_x(b, c):
        u, size = unit_of(b, c), blocks[b]
        for e in range(1, inner):
            src, dst = x_send.at[u, e - 1, pl.ds(0, size)], x_recv.at[u, e - 1, pl.ds(0, size)]
            x_send[u, e - 1, :size] = product(b, c, e).astype(BF16)
            send(src, dst, x_s.at[u, e - 1], x_r.at[u, e - 1], pz * inner + x_at(e), s)

    @scoped
    def stage_z(b, c):
        u, size = unit_of(b, c), blocks[b]
        q = size // outer
        grads[u, :size] = product(b, c, 0)
        for e in range(1, inner):
            arrived(x_recv.at[u, e - 1, pl.ds(0, size)], x_s.at[u, e - 1], x_r.at[u, e - 1])

        def sum_of(z):
            rows = pl.ds(pl.multiple_of(z * q, 16), q)
            value = grads[u, rows, :]
            for e in range(1, inner):
                value = value + x_recv[u, e - 1, rows, :].astype(F32)
            return value
        for k in range(1, outer):
            to = z_to(k)
            value = sum_of(to)
            if k == 1:
                z_near[u, :q] = value
                src, dst = z_near.at[u, pl.ds(0, q)], z_near_recv.at[u, pl.ds(0, q)]
            else:
                z_far[u, k - 2, :q] = value.astype(BF16)
                src, dst = z_far.at[u, k - 2, pl.ds(0, q)], z_far_recv.at[u, k - 2, pl.ds(0, q)]
            send(src, dst, z_s.at[u, k - 1], z_r.at[u, k - 1], to * inner + px, s)
        z_own[u, :q] = sum_of(pz)

    line = outer == 4
    far = 2 - 2 * (pz // 2)
    middle = (pz == 1) | (pz == 2)

    def out_spot(b, c, z):
        q = blocks[b] // outer
        return out.at[pl.ds(pl.multiple_of(px * hrows + starts[b] + z * q, 16), q), lanes_of(c)]

    def out_half(b, c, x):
        return out.at[pl.ds(pl.multiple_of(x * hrows + starts[b], 128), blocks[b]), lanes_of(c)]

    @scoped
    def stage_sum(b, c):
        u, q = unit_of(b, c), blocks[b] // outer
        value = z_own[u, :q]
        for k in range(1, outer):
            dst = z_near_recv.at[u, pl.ds(0, q)] if k == 1 else z_far_recv.at[u, k - 2, pl.ds(0, q)]
            arrived(dst, z_s.at[u, k - 1], z_r.at[u, k - 1])
            value = value + dst[...].astype(F32)
        spot = out_spot(b, c, pz)
        spot[...] = value.astype(BF16)
        if line:
            send(spot, spot, az_s.at[u, 0], az_r.at[u, 0], z_to(1) * inner + px, s)
            i = 1 + lax.rem(pz, 2)
            send(spot, spot, az_s.at[u, i], az_r.at[u, i], (2 - pz // 2) * inner + px, s)
        else:
            for k in range(1, outer):
                send(spot, spot, az_s.at[u, k - 1], az_r.at[u, k - 1], z_to(k) * inner + px, s)

    def far_copy(b, c):
        q = blocks[b] // outer
        first = px * hrows + starts[b] + far * q
        spot = out.at[pl.ds(pl.multiple_of(first, 16), 2 * q), lanes_of(c)]
        u = unit_of(b, c)
        return pltpu.make_async_remote_copy(
            src_ref=spot, dst_ref=spot, send_sem=af_s.at[u], recv_sem=af_r.at[u],
            device_id=(z_to(1) * inner + px, s), device_id_type=MESH,
        )

    @scoped
    def stage_far(b, c):
        if line:
            u = unit_of(b, c)

            @pl.when(middle)
            def _():
                for i in range(2):
                    arrived(out_spot(b, c, far + i), az_s.at[u, 1 + i], az_r.at[u, 1 + i])
                far_copy(b, c).start()

    @scoped
    def stage_relay(b, c):
        u = unit_of(b, c)
        if line:
            arrived(out_spot(b, c, z_to(1)), az_s.at[u, 0], az_r.at[u, 0])

            @pl.when(jnp.logical_not(middle))
            def _():
                far_copy(b, c).wait_recv()
        else:
            for k in range(1, outer):
                arrived(out_spot(b, c, z_from(k)), az_s.at[u, k - 1], az_r.at[u, k - 1])
        spot = out_half(b, c, px)
        for e in range(1, inner):
            send(spot, spot, ax_s.at[u, e - 1], ax_r.at[u, e - 1], pz * inner + x_at(e), s)

    @scoped
    def stage_settle(b, c):
        u = unit_of(b, c)
        for e in range(1, inner):
            arrived(out_half(b, c, x_at(-e)), ax_s.at[u, e - 1], ax_r.at[u, e - 1])

    turn(n_own.at[s], s, 0, feats)
    from_members(cnt_m, cnt_s, cnt_r)
    cnt_g[p] = total_of(cnt_m, members)
    to_groups(cnt_g, cntg_s, cntg_r)
    if chunks > 1:
        w_spread(1)
    w_relay(0)
    arrived(n_recv.at[twin], n_s.at[t_slot], n_r.at[t_slot])
    turn(n_recv.at[twin], twin, 0, feats)
    from_groups(cnt_g, cntg_s, cntg_r)
    total = total_of(cnt_g, groups)
    position = lax.broadcasted_iota(jnp.int32, (tokens, 1), 0)
    valid = jnp.where(position < rows_count * is_alive, 1.0, 0.0).astype(F32)
    scale = valid * (SCALE / total[:1, :1])

    loss = jnp.zeros((1, kc), F32)
    keyed, passed, landed = [0], [], []

    def next_keys(loss):
        c = keyed[0]
        if c + 2 < chunks:
            w_spread(c + 2)
        if c + 1 < chunks:
            w_relay(c + 1)
        w_settle(c)
        loss = stage_keys(c, loss)
        keyed[0] += 1
        if keyed[0] == chunks:
            loss_m[s] = jnp.broadcast_to(jnp.sum(loss, axis=1, keepdims=True), (8, 128))
            to_members(loss_m, loss_s, loss_r)
        return loss

    def ready(b, c):
        if b not in landed:
            landed.append(b)
            n_land(b)
        if c not in passed:
            passed.append(c)
            dk_pass(c)
            dk_ready(c)

    units = plan_of(len(blocks), chunks)
    def keys_and_columns(loss, count):
        while keyed[0] < count:
            loss = next_keys(loss)
            for b in range(1, len(blocks)):
                if min(SEND_AFTER[min(b, 2)], chunks) == keyed[0]:
                    n_send(b)
        return loss
    loss = keys_and_columns(loss, min(KEYS_AHEAD, chunks))
    stages = {"X": stage_x, "Z": stage_z, "S": stage_sum, "F": stage_far, "R": stage_relay}
    for name, i in order_of(units):
        if name == "K":
            loss = keys_and_columns(loss, chunks)
        elif name == "L":
            from_members(loss_m, loss_s, loss_r)
            loss_g[p] = total_of(loss_m, members)
            to_groups(loss_g, lossg_s, lossg_r)
        else:
            if name == "X":
                ready(*units[i])
            stages[name](*units[i])
    from_groups(loss_g, lossg_s, lossg_r)
    loss_out[0, 0] = (total_of(loss_g, groups) / (2.0 * kv * total))[0, 0]
    for unit in units:
        if unit:
            stage_settle(*unit)
    with jax.named_scope("drain"):
        for copy in pending:
            copy.wait_send()
        if line:
            @pl.when(middle)
            def _():
                for b, c in filter(None, units):
                    far_copy(b, c).wait_send()


def body(members, groups, hidden_in, teacher, norm_gain, w_key, group_rows, member):
    tokens, width = hidden_in.shape
    owned, kv = w_key.shape
    inner = inner_of(groups)
    outer = groups // inner
    unit = math.lcm(128 * inner, 16 * groups)
    feats = -(-owned // unit) * unit
    blocks = blocks_of(feats // inner)
    units, most = len(blocks) * (kv // 256 if kv % 256 == 0 else 1), max(blocks)
    chunks = kv // 256 if kv % 256 == 0 else 1
    kc = kv // chunks
    gains = norm_gain.astype(F32)
    hidden, weights, wide_gains = hidden_in, w_key, norm_gain
    if feats != owned:
        extra = feats - owned
        hidden = jnp.pad(hidden_in.reshape(tokens, members, owned), ((0, 0), (0, 0), (0, extra)))
        hidden = hidden.reshape(tokens, members * feats)
        weights = jnp.pad(w_key, ((0, extra), (0, 0)))
        wide_gains = jnp.pad(norm_gain, (0, extra))
    pairs = members // 2
    vm = pltpu.VMEM

    def some(n):
        return max(n, 1)

    def sems(*shape):
        kind = pltpu.SemaphoreType.DMA(tuple(some(n) for n in shape))
        return [kind, kind]

    small = lambda n: vm((n, 8, 128), F32)
    space = pltpu.MemorySpace
    grad, loss = pl.pallas_call(
        functools.partial(kernel, members, groups, width, chunks, blocks),
        out_shape=(
            jax.ShapeDtypeStruct((feats, kv), BF16),
            jax.ShapeDtypeStruct((1, 1), F32),
        ),
        in_specs=[
            pl.BlockSpec(memory_space=pltpu.SMEM),
            pl.BlockSpec(memory_space=pltpu.SMEM),
            pl.BlockSpec(memory_space=pl.ANY),
            pl.BlockSpec(memory_space=pltpu.VMEM),
            pl.BlockSpec(memory_space=pltpu.VMEM),
            pl.BlockSpec(memory_space=pl.ANY),
        ],
        out_specs=(pl.BlockSpec(memory_space=pltpu.VMEM), pl.BlockSpec(memory_space=pltpu.SMEM)),
        scratch_shapes=[
            vm((tokens, members * feats), BF16),
            vm((chunks, members, feats, kc), BF16),
            vm((members, 1, feats), F32),
            small(members), small(groups), small(members), small(groups),
            vm((members, tokens, feats), BF16), vm((members, tokens, feats), BF16),
            vm((feats, members * tokens), BF16),
            vm((chunks, members, tokens, kc), BF16),
            vm((units, most, kc), F32),
            vm((units, some(inner - 1), most, kc), BF16), vm((units, some(inner - 1), most, kc), BF16),
            vm((units, most // outer, kc), F32), vm((units, most // outer, kc), F32),
            vm((units, some(outer - 2), most // outer, kc), BF16),
            vm((units, some(outer - 2), most // outer, kc), BF16),
            vm((units, most // outer, kc), F32),
            sems(chunks + 1)[0],
            *sems(members - 1), *sems(members - 1), *sems(groups - 1),
            *sems(members - 1), *sems(groups - 1),
            *sems(chunks, pairs - 1),
            *sems(chunks * (pairs - 1), inner), *sems(chunks * (pairs - 1), inner - 1, 2),
            *sems(chunks, pairs),
            *sems((pairs - 1) * 2 * inner * len(blocks) + 1),
            *sems(chunks, pairs - 1), *sems(chunks), *sems(chunks, pairs - 1),
            *sems(units, inner - 1), *sems(units, outer - 1),
            *sems(units, outer - 1), *sems(units), *sems(units, inner - 1),
        ],
        compiler_params=pltpu.CompilerParams(
            collective_id=0, has_side_effects=True, vmem_limit_bytes=60 * 1024 * 1024
        ),
    )(group_rows, member, hidden, teacher, wide_gains, weights)
    grad_key = grad[:owned].astype(F32)
    grad_gain = jnp.sum(grad_key * w_key.astype(F32), axis=1) / gains
    return (loss[0, 0], grad_gain, grad_key)


def solution(mesh):
    in_specs = (
        P(("dp", "shard"), None),
        P(("dp", "shard"), None),
        P("shard"),
        P("shard", None),
        P("dp"),
        P("dp", "shard"),
    )
    out_specs = (P(), P("shard"), P("shard", None))
    step = functools.partial(body, mesh.shape["shard"], mesh.shape["dp"])
    return jax.shard_map(step, mesh=mesh, in_specs=in_specs, out_specs=out_specs, check_vma=False)
```

```python
import functools
import math

import jax
import jax.numpy as jnp
from jax import lax
from jax.experimental import pallas as pl
from jax.experimental.pallas import tpu as pltpu
from jax.sharding import PartitionSpec as P

EPSILON = 1e-06
SCALE = 1024.0
MESH = pl.DeviceIdType.MESH
F32 = jnp.float32
BF16 = jnp.bfloat16


def inner_of(groups):
    return max(d for d in range(1, groups + 1) if groups % d == 0 and d * d <= groups)


def blocks_of(rows):
    unit = 128
    count = rows // unit
    if count == sum(SHARES):
        return [n * unit for n in SHARES]
    return [min(2, count - i) * unit for i in range(0, count, 2)]


SHARES, SEND_AFTER = (2, 1, 2), (0, 1, 3)
KEYS_AHEAD = 2
LAGS = (0, 2, 4, 6, 7)


def order_of(units):
    order = []
    for i in range(len(units) + LAGS[-1]):
        for lag, name in reversed(tuple(zip(LAGS, "XZSFR"))):
            if 0 <= i - lag < len(units):
                order.append((name, i - lag))
        if i == 0:
            order.append(("K", 0))
        if i == len(units) - 1:
            order.append(("L", 0))
    return order


def plan_of(blocks, chunks):
    early = max(blocks - 1, 1)
    first = [(b, c) for c in range(chunks) for b in range(early)]
    return first + [(b, c) for b in range(early, blocks) for c in range(chunks)]


def paired(index, k, size):
    if size & (size - 1):
        return None
    out, bit = 0, 1
    while bit < size:
        out = out + lax.rem(lax.rem(index // bit, 2) + (k // bit) % 2, 2) * bit
        bit *= 2
    return out


def kernel(
    members, groups, width, chunks, blocks,
    live_rows, alive, hidden_in, teacher, gains, w_in,
    out, loss_out,
    hidden, w_full, gains_all, cnt_m, cnt_g, loss_m, loss_g,
    n_own, n_recv, n_t, dk_all, grads,
    x_send, x_recv, z_near, z_near_recv, z_far, z_far_recv, z_own,
    load_s, gain_s, gain_r, cnt_s, cnt_r, cntg_s, cntg_r,
    loss_s, loss_r, lossg_s, lossg_r, wy_s, wy_r, wz_s, wz_r, wx_s, wx_r, wt_s, wt_r,
    n_s, n_r, dk_s, dk_r, dks_s, dks_r, dkf_s, dkf_r,
    x_s, x_r, z_s, z_r, az_s, az_r, af_s, af_r, ax_s, ax_r,
):
    tokens, kv = teacher.shape
    feats = w_in.shape[0]
    kc = kv // chunks
    inner = inner_of(groups)
    outer = groups // inner
    hrows = feats // inner
    qrows = hrows // outer
    pairs = members // 2
    starts = [sum(blocks[:b]) for b in range(len(blocks))]
    p, s = lax.axis_index("dp"), lax.axis_index("shard")
    px, pz = lax.rem(p, inner), p // inner
    chip, par = s // 2, lax.rem(s, 2)
    twin = chip * 2 + 1 - par
    pending = []

    def scoped(stage):
        def run(c, *rest):
            with jax.named_scope("_".join([stage.__name__, str(c), *[str(r) for r in rest if isinstance(r, int)]])):
                return stage(c, *rest)
        return run

    def member_at(d):
        return lax.rem(s + d, members)

    def group_at(d):
        return lax.rem(p + d, groups)

    def chip_at(d):
        return lax.rem(chip + d + pairs, pairs)

    def x_at(d):
        return lax.rem(px + d + inner, inner)

    def z_to(k):
        q = paired(pz, k, outer)
        return lax.rem(pz + k, outer) if q is None else q

    def z_from(k):
        q = paired(pz, k, outer)
        return lax.rem(pz + outer - k, outer) if q is None else q

    def send(src, dst, ssem, rsem, group, member):
        copy = pltpu.make_async_remote_copy(
            src_ref=src, dst_ref=dst, send_sem=ssem, recv_sem=rsem,
            device_id=(group, member), device_id_type=MESH,
        )
        copy.start()
        pending.append(copy)

    def arrived(dst, ssem, rsem):
        pltpu.make_async_remote_copy(
            src_ref=dst, dst_ref=dst, send_sem=ssem, recv_sem=rsem,
            device_id=(p, twin), device_id_type=MESH,
        ).wait_recv()

    def lanes_of(c):
        return pl.ds(c * kc, kc)

    def rows_at(x, z):
        return pl.ds(pl.multiple_of(x * hrows + z * qrows, 16), qrows)

    loads = [
        pltpu.make_async_copy(w_in.at[:, lanes_of(c)], w_full.at[c, s], load_s.at[c])
        for c in range(chunks)
    ]
    loads.append(pltpu.make_async_copy(hidden_in, hidden, load_s.at[chunks]))
    for copy in loads:
        copy.start()

    rows_count, is_alive = live_rows[0], alive[0, 0]
    gains_all[s] = gains[...].astype(F32).reshape(1, feats)
    cnt_m[s] = jnp.broadcast_to((is_alive * rows_count).astype(F32), (8, 128))

    barrier = pltpu.get_barrier_semaphore()
    for d in range(1, members):
        pl.semaphore_signal(barrier, inc=1, device_id=(p, member_at(d)), device_id_type=MESH)
    for d in range(1, groups):
        pl.semaphore_signal(barrier, inc=1, device_id=(group_at(d), s), device_id_type=MESH)
    pl.semaphore_wait(barrier, members + groups - 2)

    def to_members(buf, ssem, rsem):
        for d in range(1, members):
            send(buf.at[s], buf.at[s], ssem.at[d - 1], rsem.at[d - 1], p, member_at(d))

    def from_members(buf, ssem, rsem):
        for d in range(1, members):
            j = lax.rem(s + members - d, members)
            arrived(buf.at[j], ssem.at[d - 1], rsem.at[d - 1])

    def to_groups(buf, ssem, rsem):
        for d in range(1, groups):
            send(buf.at[p], buf.at[p], ssem.at[d - 1], rsem.at[d - 1], group_at(d), s)

    def from_groups(buf, ssem, rsem):
        for d in range(1, groups):
            j = lax.rem(p + groups - d, groups)
            arrived(buf.at[j], ssem.at[d - 1], rsem.at[d - 1])

    def total_of(buf, n):
        value = buf[0]
        for i in range(1, n):
            value = value + buf[i]
        return value

    to_members(gains_all, gain_s, gain_r)
    to_members(cnt_m, cnt_s, cnt_r)

    half = 2 if outer % 2 == 0 else 1
    hz = lax.rem(pz, half)
    hz_other = half - 1 - hz
    z_pair = (pz - hz + hz_other) * inner + px
    wrows = feats // (inner * half)

    def w_spot(c, j, x, h):
        return w_full.at[c, j, pl.ds(pl.multiple_of((x * half + h) * wrows, 16), wrows), :]

    @scoped
    def w_own(c):
        loads[c].wait()
        spot = w_spot(c, s, px, hz)
        for d in range(1, pairs):
            send(spot, spot, wy_s.at[c, d - 1], wy_r.at[c, d - 1], p, chip_at(d) * 2 + par)
        send(w_full.at[c, s], w_full.at[c, s], wt_s.at[c, 0], wt_r.at[c, 0], p, twin)

    def w_index(c, d):
        return c * (pairs - 1) + d - 1

    def w_sources():
        return [(d, chip_at(-d) * 2 + par) for d in range(1, pairs)]

    def w_to_x(spot, i, k):
        for e in range(1, inner):
            send(spot, spot, wx_s.at[i, e - 1, k], wx_r.at[i, e - 1, k], pz * inner + x_at(e), s)

    def w_to_z(spot, i, e):
        if half == 2:
            send(spot, spot, wz_s.at[i, e], wz_r.at[i, e], z_pair, s)

    def z_first(c):
        return c % 2 == 1

    @scoped
    def w_spread(c):
        for d, j in w_sources():
            i = w_index(c, d)
            spot = w_spot(c, j, px, hz)
            arrived(spot, wy_s.at[c, d - 1], wy_r.at[c, d - 1])
            w_to_z(spot, i, 0)
            w_to_x(spot, i, 0)

    @scoped
    def w_relay(c):
        for d, j in w_sources():
            i = w_index(c, d)
            if half == 1:
                continue
            if z_first(c):
                spot = w_spot(c, j, px, hz_other)
                arrived(spot, wz_s.at[i, 0], wz_r.at[i, 0])
                w_to_x(spot, i, 1)
            else:
                for e in range(1, inner):
                    spot = w_spot(c, j, x_at(-e), hz)
                    arrived(spot, wx_s.at[i, e - 1, 0], wx_r.at[i, e - 1, 0])
                    w_to_z(spot, i, e)

    @scoped
    def w_settle(c):
        for d, j in w_sources():
            i = w_index(c, d)
            if half == 1 or z_first(c):
                for k in range(half):
                    for e in range(1, inner):
                        h = hz_other if k else hz
                        arrived(w_spot(c, j, x_at(-e), h), wx_s.at[i, e - 1, k], wx_r.at[i, e - 1, k])
            else:
                for e in range(inner):
                    arrived(w_spot(c, j, x_at(-e), hz_other), wz_s.at[i, e], wz_r.at[i, e])
            send(w_full.at[c, j], w_full.at[c, j], wt_s.at[c, d], wt_r.at[c, d], p, twin)

    def w_ready(c):
        for d in range(pairs):
            j = chip_at(-d) * 2 + 1 - par
            arrived(w_full.at[c, j], wt_s.at[c, d], wt_r.at[c, d])

    for c in range(chunks):
        w_own(c)

    def part_of(e, b):
        return pl.ds(pl.multiple_of(x_at(e) * hrows + starts[b], 128), blocks[b])

    def n_index(d, h, b):
        return (((d - 1) * 2 + h) * len(blocks) + b) * inner

    with jax.named_scope("hidden"):
        loads[chunks].wait()
    step_rows = 32
    from_members(gains_all, gain_s, gain_r)

    def normalise(r, carry):
        rows = pl.ds(pl.multiple_of(r * step_rows, step_rows), step_rows)
        square = jnp.zeros((step_rows, 1), F32)
        for j in range(members):
            x = hidden[rows, pl.ds(j * feats, feats)].astype(F32)
            square = square + jnp.sum(x * x, axis=1, keepdims=True)
        inv = lax.rsqrt(square / width + EPSILON)
        for j in range(members):
            x = hidden[rows, pl.ds(j * feats, feats)].astype(F32)
            n_own[j, rows, :] = (x * inv * gains_all[j]).astype(BF16)
        return carry
    w_spread(0)
    with jax.named_scope("normalise"):
        lax.fori_loop(0, tokens // step_rows, normalise, 0)

    @scoped
    def n_send(b):
        for e in [*range(1, inner), 0]:
            for d in range(1, pairs):
                for h in range(2):
                    j = chip_at(d) * 2 + lax.rem(par + h, 2)
                    i = n_index(d, h, b) + e
                    send(n_own.at[j, :, part_of(e, b)], n_recv.at[s, :, part_of(e, b)], n_s.at[i], n_r.at[i], p, j)

    n_send(0)
    t_slot = (pairs - 1) * 2 * inner * len(blocks)
    send(n_own.at[twin], n_recv.at[s], n_s.at[t_slot], n_r.at[t_slot], p, twin)

    def turn(source, m, first, count):
        def step(b, carry):
            lanes = pl.ds(pl.multiple_of(first + b * 128, 128), 128)
            n_t[lanes, pl.ds(pl.multiple_of(m * tokens, 128), tokens)] = source[:, lanes].T
            return carry
        with jax.named_scope("turn"):
            lax.fori_loop(0, count // 128, step, 0)

    @scoped
    def n_land(b):
        for e in [*range(1, inner), 0]:
            for d in range(1, pairs):
                for h in range(2):
                    m = chip_at(-d) * 2 + lax.rem(par + h, 2)
                    i = n_index(d, h, b) + e
                    arrived(n_recv.at[m, :, part_of(e, b)], n_s.at[i], n_r.at[i])
                    turn(n_recv.at[m], m, x_at(e) * hrows + starts[b], blocks[b])

    @scoped
    def stage_keys(c, loss):
        w_ready(c)
        keys = jnp.dot(n_own[0], w_full[c, 0], preferred_element_type=F32)
        for j in range(1, members):
            keys = keys + jnp.dot(n_own[j], w_full[c, j], preferred_element_type=F32)
        diff = keys - teacher[:, lanes_of(c)].astype(F32)
        dk_all[c, s] = (scale * diff).astype(BF16)
        for d in range(1, pairs):
            send(
                dk_all.at[c, s], dk_all.at[c, s], dk_s.at[c, d - 1], dk_r.at[c, d - 1],
                p, chip_at(d) * 2 + par,
            )
        send(dk_all.at[c, s], dk_all.at[c, s], dks_s.at[c], dks_r.at[c], p, twin)
        return loss + jnp.sum(valid * diff * diff, axis=0, keepdims=True)

    @scoped
    def dk_pass(c):
        for d in range(1, pairs):
            q = chip_at(-d) * 2 + par
            arrived(dk_all.at[c, q], dk_s.at[c, d - 1], dk_r.at[c, d - 1])
            send(dk_all.at[c, q], dk_all.at[c, q], dkf_s.at[c, d - 1], dkf_r.at[c, d - 1], p, twin)

    def dk_ready(c):
        arrived(dk_all.at[c, twin], dks_s.at[c], dks_r.at[c])
        for d in range(1, pairs):
            q = chip_at(-d) * 2 + 1 - par
            arrived(dk_all.at[c, q], dkf_s.at[c, d - 1], dkf_r.at[c, d - 1])

    def product(b, c, e):
        dk = dk_all[c].reshape(members * tokens, kc)
        return jnp.dot(n_t[part_of(e, b), :], dk, preferred_element_type=F32)

    def unit_of(b, c):
        return b * chunks + c

    @scoped
    def stage_x(b, c):
        u, size = unit_of(b, c), blocks[b]
        for e in range(1, inner):
            src, dst = x_send.at[u, e - 1, pl.ds(0, size)], x_recv.at[u, e - 1, pl.ds(0, size)]
            x_send[u, e - 1, :size] = product(b, c, e).astype(BF16)
            send(src, dst, x_s.at[u, e - 1], x_r.at[u, e - 1], pz * inner + x_at(e), s)

    @scoped
    def stage_z(b, c):
        u, size = unit_of(b, c), blocks[b]
        q = size // outer
        grads[u, :size] = product(b, c, 0)
        for e in range(1, inner):
            arrived(x_recv.at[u, e - 1, pl.ds(0, size)], x_s.at[u, e - 1], x_r.at[u, e - 1])

        def sum_of(z):
            rows = pl.ds(pl.multiple_of(z * q, 16), q)
            value = grads[u, rows, :]
            for e in range(1, inner):
                value = value + x_recv[u, e - 1, rows, :].astype(F32)
            return value
        for k in range(1, outer):
            to = z_to(k)
            value = sum_of(to)
            if k == 1:
                z_near[u, :q] = value
                src, dst = z_near.at[u, pl.ds(0, q)], z_near_recv.at[u, pl.ds(0, q)]
            else:
                z_far[u, k - 2, :q] = value.astype(BF16)
                src, dst = z_far.at[u, k - 2, pl.ds(0, q)], z_far_recv.at[u, k - 2, pl.ds(0, q)]
            send(src, dst, z_s.at[u, k - 1], z_r.at[u, k - 1], to * inner + px, s)
        z_own[u, :q] = sum_of(pz)

    line = outer == 4
    far = 2 - 2 * (pz // 2)
    middle = (pz == 1) | (pz == 2)

    def out_spot(b, c, z):
        q = blocks[b] // outer
        return out.at[pl.ds(pl.multiple_of(px * hrows + starts[b] + z * q, 16), q), lanes_of(c)]

    def out_half(b, c, x):
        return out.at[pl.ds(pl.multiple_of(x * hrows + starts[b], 128), blocks[b]), lanes_of(c)]

    @scoped
    def stage_sum(b, c):
        u, q = unit_of(b, c), blocks[b] // outer
        value = z_own[u, :q]
        for k in range(1, outer):
            dst = z_near_recv.at[u, pl.ds(0, q)] if k == 1 else z_far_recv.at[u, k - 2, pl.ds(0, q)]
            arrived(dst, z_s.at[u, k - 1], z_r.at[u, k - 1])
            value = value + dst[...].astype(F32)
        spot = out_spot(b, c, pz)
        spot[...] = value.astype(BF16)
        if line:
            send(spot, spot, az_s.at[u, 0], az_r.at[u, 0], z_to(1) * inner + px, s)
            i = 1 + lax.rem(pz, 2)
            send(spot, spot, az_s.at[u, i], az_r.at[u, i], (2 - pz // 2) * inner + px, s)
        else:
            for k in range(1, outer):
                send(spot, spot, az_s.at[u, k - 1], az_r.at[u, k - 1], z_to(k) * inner + px, s)

    def far_copy(b, c):
        q = blocks[b] // outer
        first = px * hrows + starts[b] + far * q
        spot = out.at[pl.ds(pl.multiple_of(first, 16), 2 * q), lanes_of(c)]
        u = unit_of(b, c)
        return pltpu.make_async_remote_copy(
            src_ref=spot, dst_ref=spot, send_sem=af_s.at[u], recv_sem=af_r.at[u],
            device_id=(z_to(1) * inner + px, s), device_id_type=MESH,
        )

    @scoped
    def stage_far(b, c):
        if line:
            u = unit_of(b, c)

            @pl.when(middle)
            def _():
                for i in range(2):
                    arrived(out_spot(b, c, far + i), az_s.at[u, 1 + i], az_r.at[u, 1 + i])
                far_copy(b, c).start()

    @scoped
    def stage_relay(b, c):
        u = unit_of(b, c)
        if line:
            arrived(out_spot(b, c, z_to(1)), az_s.at[u, 0], az_r.at[u, 0])

            @pl.when(jnp.logical_not(middle))
            def _():
                far_copy(b, c).wait_recv()
        else:
            for k in range(1, outer):
                arrived(out_spot(b, c, z_from(k)), az_s.at[u, k - 1], az_r.at[u, k - 1])
        spot = out_half(b, c, px)
        for e in range(1, inner):
            send(spot, spot, ax_s.at[u, e - 1], ax_r.at[u, e - 1], pz * inner + x_at(e), s)

    @scoped
    def stage_settle(b, c):
        u = unit_of(b, c)
        for e in range(1, inner):
            arrived(out_half(b, c, x_at(-e)), ax_s.at[u, e - 1], ax_r.at[u, e - 1])

    turn(n_own.at[s], s, 0, feats)
    from_members(cnt_m, cnt_s, cnt_r)
    cnt_g[p] = total_of(cnt_m, members)
    to_groups(cnt_g, cntg_s, cntg_r)
    if chunks > 1:
        w_spread(1)
    w_relay(0)
    arrived(n_recv.at[twin], n_s.at[t_slot], n_r.at[t_slot])
    turn(n_recv.at[twin], twin, 0, feats)
    from_groups(cnt_g, cntg_s, cntg_r)
    total = total_of(cnt_g, groups)
    position = lax.broadcasted_iota(jnp.int32, (tokens, 1), 0)
    valid = jnp.where(position < rows_count * is_alive, 1.0, 0.0).astype(F32)
    scale = valid * (SCALE / total[:1, :1])

    loss = jnp.zeros((1, kc), F32)
    keyed, passed, landed = [0], [], []

    def next_keys(loss):
        c = keyed[0]
        if c + 2 < chunks:
            w_spread(c + 2)
        if c + 1 < chunks:
            w_relay(c + 1)
        w_settle(c)
        loss = stage_keys(c, loss)
        keyed[0] += 1
        if keyed[0] == chunks:
            loss_m[s] = jnp.broadcast_to(jnp.sum(loss, axis=1, keepdims=True), (8, 128))
            to_members(loss_m, loss_s, loss_r)
        return loss

    def ready(b, c):
        if b not in landed:
            landed.append(b)
            n_land(b)
        if c not in passed:
            passed.append(c)
            dk_pass(c)
            dk_ready(c)

    units = plan_of(len(blocks), chunks)
    def keys_and_columns(loss, count):
        while keyed[0] < count:
            loss = next_keys(loss)
            for b in range(1, len(blocks)):
                if min(SEND_AFTER[min(b, 2)], chunks) == keyed[0]:
                    n_send(b)
        return loss
    loss = keys_and_columns(loss, min(KEYS_AHEAD, chunks))
    stages = {"X": stage_x, "Z": stage_z, "S": stage_sum, "F": stage_far, "R": stage_relay}
    for name, i in order_of(units):
        if name == "K":
            loss = keys_and_columns(loss, chunks)
        elif name == "L":
            from_members(loss_m, loss_s, loss_r)
            loss_g[p] = total_of(loss_m, members)
            to_groups(loss_g, lossg_s, lossg_r)
        else:
            if name == "X":
                ready(*units[i])
            stages[name](*units[i])
    from_groups(loss_g, lossg_s, lossg_r)
    loss_out[0, 0] = (total_of(loss_g, groups) / (2.0 * kv * total))[0, 0]
    for unit in units:
        if unit:
            stage_settle(*unit)
    with jax.named_scope("drain"):
        for copy in pending:
            copy.wait_send()
        if line:
            @pl.when(middle)
            def _():
                for b, c in filter(None, units):
                    far_copy(b, c).wait_send()


def body(members, groups, hidden_in, teacher, norm_gain, w_key, group_rows, member):
    tokens, width = hidden_in.shape
    owned, kv = w_key.shape
    inner = inner_of(groups)
    outer = groups // inner
    unit = math.lcm(128 * inner, 16 * groups)
    feats = -(-owned // unit) * unit
    blocks = blocks_of(feats // inner)
    units, most = len(blocks) * (kv // 256 if kv % 256 == 0 else 1), max(blocks)
    chunks = kv // 256 if kv % 256 == 0 else 1
    kc = kv // chunks
    gains = norm_gain.astype(F32)
    hidden, weights, wide_gains = hidden_in, w_key, norm_gain
    if feats != owned:
        extra = feats - owned
        hidden = jnp.pad(hidden_in.reshape(tokens, members, owned), ((0, 0), (0, 0), (0, extra)))
        hidden = hidden.reshape(tokens, members * feats)
        weights = jnp.pad(w_key, ((0, extra), (0, 0)))
        wide_gains = jnp.pad(norm_gain, (0, extra))
    pairs = members // 2
    vm = pltpu.VMEM

    def some(n):
        return max(n, 1)

    def sems(*shape):
        kind = pltpu.SemaphoreType.DMA(tuple(some(n) for n in shape))
        return [kind, kind]

    small = lambda n: vm((n, 8, 128), F32)
    space = pltpu.MemorySpace
    grad, loss = pl.pallas_call(
        functools.partial(kernel, members, groups, width, chunks, blocks),
        out_shape=(
            jax.ShapeDtypeStruct((feats, kv), BF16),
            jax.ShapeDtypeStruct((1, 1), F32),
        ),
        in_specs=[
            pl.BlockSpec(memory_space=pltpu.SMEM),
            pl.BlockSpec(memory_space=pltpu.SMEM),
            pl.BlockSpec(memory_space=pl.ANY),
            pl.BlockSpec(memory_space=pltpu.VMEM),
            pl.BlockSpec(memory_space=pltpu.VMEM),
            pl.BlockSpec(memory_space=pl.ANY),
        ],
        out_specs=(pl.BlockSpec(memory_space=pltpu.VMEM), pl.BlockSpec(memory_space=pltpu.SMEM)),
        scratch_shapes=[
            vm((tokens, members * feats), BF16),
            vm((chunks, members, feats, kc), BF16),
            vm((members, 1, feats), F32),
            small(members), small(groups), small(members), small(groups),
            vm((members, tokens, feats), BF16), vm((members, tokens, feats), BF16),
            vm((feats, members * tokens), BF16),
            vm((chunks, members, tokens, kc), BF16),
            vm((units, most, kc), F32),
            vm((units, some(inner - 1), most, kc), BF16), vm((units, some(inner - 1), most, kc), BF16),
            vm((units, most // outer, kc), F32), vm((units, most // outer, kc), F32),
            vm((units, some(outer - 2), most // outer, kc), BF16),
            vm((units, some(outer - 2), most // outer, kc), BF16),
            vm((units, most // outer, kc), F32),
            sems(chunks + 1)[0],
            *sems(members - 1), *sems(members - 1), *sems(groups - 1),
            *sems(members - 1), *sems(groups - 1),
            *sems(chunks, pairs - 1),
            *sems(chunks * (pairs - 1), inner), *sems(chunks * (pairs - 1), inner - 1, 2),
            *sems(chunks, pairs),
            *sems((pairs - 1) * 2 * inner * len(blocks) + 1),
            *sems(chunks, pairs - 1), *sems(chunks), *sems(chunks, pairs - 1),
            *sems(units, inner - 1), *sems(units, outer - 1),
            *sems(units, outer - 1), *sems(units), *sems(units, inner - 1),
        ],
        compiler_params=pltpu.CompilerParams(
            collective_id=0, has_side_effects=True, vmem_limit_bytes=60 * 1024 * 1024
        ),
    )(group_rows, member, hidden, teacher, wide_gains, weights)
    grad_key = grad[:owned].astype(F32)
    grad_gain = jnp.sum(grad_key * w_key.astype(F32), axis=1) / gains
    return (loss[0, 0], grad_gain, grad_key)


def solution(mesh):
    in_specs = (
        P(("dp", "shard"), None),
        P(("dp", "shard"), None),
        P("shard"),
        P("shard", None),
        P("dp"),
        P("dp", "shard"),
    )
    out_specs = (P(), P("shard"), P("shard", None))
    step = functools.partial(body, mesh.shape["shard"], mesh.shape["dp"])
    return jax.shard_map(step, mesh=mesh, in_specs=in_specs, out_specs=out_specs, check_vma=False)
```
